256 devices in a mesh: grid: 32 (over z, y), atom: 8 (over x, core).
Axes of the slice: x: 4, y: 4, z: 8, core: 2. Of those that a mesh axis runs over, the one named last changes fastest.
Arguments:
- weights: float32 [4194304], P(('grid', 'atom')), may hold values from 0.25 to 4
- target: float32 [4194304], P(('grid', 'atom')), may hold values from -6 to 6
- coupling: float32 [4194304], P(('grid', 'atom')), may hold values from -0.9 to 0.9
- multipole_basis: float32 [25, 4194304], P(None, ('grid', 'atom')), may hold values from -6 to 6
- rho_hist: float32 [8, 4194304], P(None, ('grid', 'atom')), may hold values from -6 to 6
- res_hist: float32 [8, 4194304], P(None, ('grid', 'atom')), may hold values from -6 to 6
- batch_atom: int32 [16384], P(('grid', 'atom')), may hold values from 0 to 4095
- owner_slot: int32 [4096], replicated, may hold values from 0 to 4095, each once
- slot_index: int32 [2], replicated, may hold values from 0 to 7
Outputs:
- density: float32 [4194304], P(('grid', 'atom'))
- moments: float32 [25, 4096], P(None, 'atom')
The draws below stay inside these ranges and needn't reach their ends.
Inputs may be any that keep to these rules, and one draw needn't show every extreme that they name: `owner_slot`: each slot 0 to 4095 belongs to exactly one atom.
All inputs are finite; a program needn't handle non-finite values.
Results may differ from the reference program's by a relative error of at most 0.00011.
Values sent between devices are 32-bit elements; how exact they have to be, the bound alone decides.
No kernel may reach another device: no remote copies, remote signals or barrier semaphores. Data moves between devices by JAX's collectives and lax.ppermute only.
A program may use at most 64 MiB of HBM per device.

```python
import math
import jax
import jax.numpy as jnp
import numpy as np
from jax import lax

H = 8
LM = 25
BATCH = 256
ITERS = 2
POINTS = 4194304
BATCHES = 16384
ATOMS = 4096
ATOM_PTS = 1024


def place_ends(result, key, least, largest):
    spot = [jax.random.randint(jax.random.fold_in(key, axis), (), 0, length) for axis, length in enumerate(result.shape)]
    longest = result.shape.index(max(result.shape))
    neighbour = spot[:longest] + [(spot[longest] + 1) % result.shape[longest]] + spot[longest + 1:]
    return result.at[tuple(spot)].set(least).at[tuple(neighbour)].set(largest)


def levels(own_key, dims, pieces, smallest, top_value):
    def one(position, shards_of):
        heights = jax.random.uniform(jax.random.fold_in(jax.random.fold_in(own_key, 6), position), (shards_of,), jnp.float32, smallest / len(pieces), top_value / len(pieces))
        return jnp.repeat(jnp.exp(heights), dims[position] // shards_of).reshape((-1,) + (1,) * (len(dims) - position - 1))

    gain = one(*pieces[0])
    for cut in pieces[1:]:
        gain = gain * one(*cut)
    return gain


def noise(stream_key, shape, scale, reach, shards=(), held_as=jnp.bfloat16):
    gain = levels(stream_key, shape, shards, -0.22, 0.18) if shards else 1.0
    entries = jax.random.normal(stream_key, shape, jnp.float32) * scale * gain
    return jnp.minimum(jnp.maximum(entries, -reach), reach).astype(held_as)


def setup_inputs(seed: int = 0) -> dict:
    splits = jax.random.split(jax.random.key(seed), 10)
    return {
        "weights": jnp.clip(jnp.exp(math.log(4.0) - 2.7725887 * jax.random.uniform(splits[0], (POINTS,), jnp.float32) ** levels(splits[0], (POINTS,), ((0, 256),), -0.2, 0.2)), 0.25, 4.0),
        "target": noise(splits[1], (POINTS,), 1.0, 6.0, ((0, 256),), jnp.float32),
        "coupling": jnp.clip(jax.random.uniform(splits[2], (POINTS,), jnp.float32, -0.9, 0.9) * levels(splits[2], (POINTS,), ((0, 256),), -0.4, 0.0), -0.9, 0.9),
        "multipole_basis": noise(splits[3], (LM, POINTS), 1.0, 6.0, ((1, 256),), jnp.float32),
        "rho_hist": noise(splits[4], (H, POINTS), 1.0, 6.0, ((1, 256),), jnp.float32),
        "res_hist": noise(splits[5], (H, POINTS), 1.0, 6.0, ((1, 256),), jnp.float32),
        "batch_atom": place_ends(jax.random.randint(splits[6], (BATCHES,), 0, ATOMS), jax.random.fold_in(splits[6], 1), 0, ATOMS - 1).astype(jnp.int32),
        "owner_slot": jax.random.permutation(splits[7], ATOMS).astype(jnp.int32),
        "slot_index": jax.random.randint(splits[8], (ITERS,), 0, H).astype(jnp.int32),
    }


damping_table = np.array([1.0 / (1 + degree) for degree in range(5) for order in range(2 * degree + 1)], dtype=np.float32)
mixing_beta = 0.5
ridge_share = 0.1

def mixing_weights(intersect):
    hist_len = intersect.shape[0]
    ridge_val = ridge_share * jnp.trace(intersect) / hist_len
    shifted = intersect + ridge_val * jnp.eye(hist_len, dtype=intersect.dtype)
    factor = jnp.linalg.cholesky(shifted)
    forward = []
    for row_at in range(hist_len):
        entry_val = 1.0
        for col_at in range(row_at):
            entry_val = entry_val - factor[row_at, col_at] * forward[col_at]
        forward.append(entry_val / factor[row_at, row_at])
    backward = [None] * hist_len
    for row_at in reversed(range(hist_len)):
        entry_val = forward[row_at]
        for col_at in range(row_at + 1, hist_len):
            entry_val = entry_val - factor[col_at, row_at] * backward[col_at]
        backward[row_at] = entry_val / factor[row_at, row_at]
    solved = jnp.stack(backward)
    return solved / jnp.sum(solved)

def reference(weights, target, coupling, multipole_basis, rho_hist, res_hist, batch_atom, owner_slot, slot_index):
    hi_prec = lax.Precision.HIGHEST
    damping = jnp.asarray(damping_table, dtype=weights.dtype)
    batch_slot = owner_slot[batch_atom].astype(jnp.int32)
    basis_blocks = multipole_basis.reshape(LM, BATCHES, BATCH)
    density = None
    moments = None
    for iteration in range(ITERS):
        intersect = jnp.dot(res_hist * weights[None, :], res_hist.T, precision=hi_prec)
        coeffs = mixing_weights(intersect)
        rho_mix = jnp.dot(coeffs, rho_hist, precision=hi_prec)
        res_mix = jnp.dot(coeffs, res_hist, precision=hi_prec)
        per_batch = lax.optimization_barrier(jnp.sum((weights * res_mix).reshape(1, BATCHES, BATCH) * basis_blocks, axis=2))
        moments = jax.ops.segment_sum(per_batch.T, batch_slot, num_segments=ATOMS).T / jnp.sqrt(jnp.float32(ATOM_PTS)).astype(weights.dtype)
        at_batch = damping[:, None] * moments[:, batch_slot]
        correct = lax.optimization_barrier(jnp.sum(at_batch[:, :, None] * basis_blocks, axis=0)).reshape(POINTS)
        density = rho_mix + mixing_beta * (res_mix - correct)
        res_new = target + coupling * jnp.tanh(density) - density
        where = slot_index[iteration]
        rho_hist = rho_hist.at[where].set(density)
        res_hist = res_hist.at[where].set(res_new)
    return (density, moments)
```

```python
import functools
import math

import jax
import jax.numpy as jnp
import numpy as np
from jax import lax
from jax.experimental import pallas as pl
from jax.experimental.pallas import tpu as pltpu
from jax.sharding import Mesh
from jax.sharding import PartitionSpec as P

ITERS = 2
AXES = ("z", "y", "x", "c")
GRID = ("z", "y")
ATOM = ("x", "c")
COL = ("z", "c")
ROW = ("y", "x")

damping_table = np.array(
    [1.0 / (1 + degree) for degree in range(5) for order in range(2 * degree + 1)], dtype=np.float32
)
mixing_beta = 0.5
ridge_share = 0.1

LANES = 128
HIST = 8
COMPS = 25
BATCHES = 64
WIDTH = 256
POINTS = BATCHES * WIDTH
PEERS = 256
SIDE = 16
KNOWN = SIDE * BATCHES
OWNED = 512

f32 = jnp.float32
bf16 = jnp.bfloat16


def iota(shape, dim):
    return lax.broadcasted_iota(jnp.int32, shape, dim)


def call(kernel, out_shape, in_specs, *, scratch=(), vmem=12 << 20, cost=20000):
    return pl.pallas_call(
        kernel,
        out_shape=out_shape,
        in_specs=[pl.BlockSpec(memory_space=s) for s in in_specs],
        out_specs=jax.tree.map(lambda _: pl.BlockSpec(memory_space=pltpu.VMEM), out_shape),
        scratch_shapes=list(scratch),
        compiler_params=pltpu.CompilerParams(vmem_limit_bytes=vmem),
        cost_estimate=pl.CostEstimate(flops=cost * 1000, bytes_accessed=1 << 20, transcendentals=0),
    )


V = pltpu.VMEM
S = pltpu.SMEM


def shape(*dims, dtype=f32):
    return jax.ShapeDtypeStruct(dims, dtype)


def gram_kernel(res, weights, slots, out):
    acc = [jnp.zeros((HIST, LANES), f32) for _ in range(5)]
    for tile in range(POINTS // LANES):
        at = pl.ds(tile * LANES, LANES)
        r = res[:, at]
        rw = r * weights[:, at]
        acc[0] += rw * r
        for d in range(1, 5):
            acc[d] += rw * pltpu.roll(r, HIST - d, 0)
    lane = iota((HIST, LANES), 1)
    sub = iota((HIST, LANES), 0)
    placed = jnp.zeros((HIST, LANES), f32)
    for d in range(HIST):
        if d < 5:
            sums = jnp.broadcast_to(jnp.sum(acc[d], axis=1, keepdims=True), (HIST, LANES))
        else:
            sums = jnp.broadcast_to(jnp.sum(acc[HIST - d], axis=1, keepdims=True), (HIST, LANES))
            sums = pltpu.roll(sums, HIST - d, 0)
        here = ((lane >> 3) == sub) & ((lane & 7) == ((sub + d) & 7))
        placed = jnp.where(here, sums, placed)
    row = jnp.sum(placed, axis=0, keepdims=True) + slots[...]
    out[...] = jnp.broadcast_to(row, (PEERS, LANES))


def solve(matrix):
    lane = iota((HIST, LANES), 1)
    sub = iota((HIST, LANES), 0)
    eye = lane == sub
    trace = jnp.sum(jnp.where(eye, matrix, 0.0), axis=(0, 1), keepdims=True)
    ridge = ridge_share * trace / HIST
    m = jnp.where(eye, matrix + ridge, matrix)
    m = jnp.where(lane == HIST, 1.0, m)
    for j in range(HIST):
        pivot_row = m[j : j + 1, :] / m[j : j + 1, j : j + 1]
        m = jnp.where(sub == j, pivot_row, m - m[:, j : j + 1] * pivot_row)
    z = m[:, HIST : HIST + 1]
    return z / jnp.sum(z, axis=0, keepdims=True)


def mixed_moments(coeffs, res, weights, basis, res_mix, out):
    c8 = jnp.broadcast_to(coeffs, (HIST, LANES))
    lane = iota((HIST, LANES), 1)
    tops = [0, 8, 16, 24]
    heights = [8, 8, 8, 1]
    acc = [jnp.zeros((h, LANES), f32) for h in heights]
    for b in range(BATCHES):
        total = [None] * 4
        for half in range(2):
            at = pl.ds(b * WIDTH + half * LANES, LANES)
            mix = jnp.sum(c8 * res[:, at], axis=0, keepdims=True)
            res_mix[:, at] = mix
            wr = mix * weights[:, at]
            for t in range(4):
                term = basis[pl.ds(tops[t], heights[t]), at] * wr
                total[t] = term if half == 0 else total[t] + term
        for t in range(4):
            sums = jnp.sum(total[t], axis=1, keepdims=True)
            place = b if t < 2 else b + BATCHES
            acc[t] = jnp.where(lane[: heights[t]] == place, sums, acc[t])
    high = jnp.where(iota((8, LANES), 0) == 0, jnp.broadcast_to(acc[3], (8, LANES)), 0.0)
    packed = jnp.concatenate([acc[0] + acc[2], acc[1] + high], axis=0)
    for peer in range(SIDE):
        out[peer] = packed


def first_mix_kernel(rows, res, weights, basis, out, res_mix, matrix_out, coeffs_out):
    row = jnp.sum(rows[...], axis=0, keepdims=True)
    wide = jnp.broadcast_to(row, (HIST, LANES))
    sub = iota((HIST, LANES), 0)
    matrix = wide
    for i in range(1, HIST):
        matrix = jnp.where(sub == i, pltpu.roll(wide, LANES - HIST * i, 1), matrix)
    matrix = jnp.where(iota((HIST, LANES), 1) < HIST, matrix, 0.0)
    matrix_out[...] = matrix
    coeffs = solve(matrix)
    coeffs_out[...] = jnp.broadcast_to(coeffs, (HIST, LANES))
    mixed_moments(coeffs, res, weights, basis, res_mix, out)


def next_mix_kernel(where, rows, matrix_in, res, weights, basis, out, res_mix, coeffs_out):
    row = jnp.broadcast_to(jnp.sum(rows[...], axis=0, keepdims=True), (HIST, LANES))
    lane = iota((HIST, LANES), 1)
    sub = iota((HIST, LANES), 0)
    slot = where[0]
    column = jnp.sum(jnp.where(lane == sub, row, 0.0), axis=1, keepdims=True)
    matrix = jnp.where(sub == slot, row, jnp.where(lane == slot, column, matrix_in[...]))
    matrix = jnp.where(lane < HIST, matrix, 0.0)
    coeffs = solve(matrix)
    coeffs_out[...] = jnp.broadcast_to(coeffs, (HIST, LANES))
    mixed_moments(coeffs, res, weights, basis, res_mix, out)


def match_kernel(place, rows, same, owned):
    z0, yx0, c0 = place[0], place[1], place[2]
    known = jnp.concatenate(
        [rows[pl.ds(z * 32 + yx0 * 2 + c, 1), :] for z in range(8) for c in range(2)], axis=0
    )
    down = jnp.transpose(known)[LANES - BATCHES :, :]
    lane1 = iota((1, LANES), 1)
    wanted = []
    for q in range(SIDE // 2):
        left = rows[pl.ds(z0 * 32 + 4 * q + c0, 1), :]
        right = rows[pl.ds(z0 * 32 + 4 * q + 2 + c0, 1), :]
        wanted.append(jnp.where(lane1 < BATCHES, pltpu.roll(left, BATCHES, 1), right))
    for i in range(SIDE):
        mine = jnp.broadcast_to(down[:, i : i + 1], (BATCHES, LANES))
        at = pl.ds(i * BATCHES, BATCHES)
        for q in range(SIDE // 2):
            hit = jnp.where(mine == wanted[q], 1.0, 0.0)
            same[at, pl.ds(q * LANES, LANES)] = hit.astype(bf16)
        for part in range(4 * OWNED // LANES):
            x, rest = divmod(part * LANES, OWNED)
            first = (2 * x + c0) * OWNED + rest
            slot = (lane1 + first).astype(f32)
            hit = jnp.where(mine == slot, 1.0, 0.0)
            owned[at, pl.ds(part * LANES, LANES)] = hit.astype(bf16)


def split3(value):
    hi = value.astype(bf16)
    rest = value - hi.astype(f32)
    mid = rest.astype(bf16)
    lo = (rest - mid.astype(f32)).astype(bf16)
    return hi, mid, lo


def gathered(pieces):
    left = iota((SIDE, LANES), 1) < BATCHES
    low, high = [], []
    for q in range(SIDE // 2):
        a, b = pieces[2 * q], pieces[2 * q + 1]
        low.append(jnp.where(left, a, pltpu.roll(b, BATCHES, 1)))
        high.append(jnp.where(left, pltpu.roll(a, BATCHES, 1), b))
    full = jnp.concatenate(
        [jnp.concatenate(low, axis=1), jnp.concatenate(high, axis=1)], axis=0
    )
    return jnp.concatenate(split3(full), axis=0)


def summed(terms, picks):
    product = jnp.dot(terms, picks, preferred_element_type=f32)
    return product[0:32] + product[32:64] + product[64:96]


def to_targets(terms, same, out):
    left = iota((SIDE, LANES), 1) < BATCHES
    sums = summed(terms, same[...])
    for q in range(SIDE // 2):
        low = sums[0:16, q * LANES : (q + 1) * LANES]
        high = sums[16:32, q * LANES : (q + 1) * LANES]
        out[2 * q, 0:16, :] = jnp.where(left, low, pltpu.roll(high, BATCHES, 1))
        out[2 * q + 1, 0:16, :] = jnp.where(left, pltpu.roll(low, BATCHES, 1), high)


def route_kernel(pieces, same, out):
    to_targets(gathered(pieces), same, out)


def last_route_kernel(pieces, same, owned, out):
    terms = gathered(pieces)
    to_targets(terms, same, out)
    for x in range(4):
        sums = summed(terms, owned[:, x * OWNED : (x + 1) * OWNED])
        for part in range(4):
            block = sums[:, part * LANES : (part + 1) * LANES]
            for y in range(4):
                out[4 * y + x, pl.ds(16 + 32 * part, 32), :] = block


def at_batches(received, scales):
    total = received[0, 0:16, :]
    for m in range(1, SIDE):
        total = total + received[m, 0:16, :]
    return jnp.concatenate([total, pltpu.roll(total, BATCHES, 1)], axis=0) * scales


def damped(scale):
    k = iota((32, LANES), 0)
    value = jnp.full((32, LANES), float(damping_table[0]), f32)
    for degree in range(1, 5):
        value = jnp.where(k >= degree * degree, float(np.float32(1.0 / (1 + degree))), value)
    return jnp.where(k < COMPS, value * scale, 0.0)


def density_tiles(at, coeffs, basis, res_mix, rho, use):
    tops = [0, 8, 16, 24]
    heights = [8, 8, 8, 1]
    for b in range(BATCHES):
        wide = [
            jnp.broadcast_to(at[tops[t] : tops[t] + heights[t], b : b + 1], (heights[t], LANES))
            for t in range(4)
        ]
        for half in range(2):
            here = pl.ds(b * WIDTH + half * LANES, LANES)
            terms = sum(wide[t] * basis[pl.ds(tops[t], 8), here] for t in range(3))
            correct = jnp.sum(terms, axis=0, keepdims=True) + wide[3] * basis[pl.ds(24, 1), here]
            rho_mix = jnp.sum(coeffs * rho[:, here], axis=0, keepdims=True)
            use(here, rho_mix + mixing_beta * (res_mix[:, here] - correct))


def update_kernel(
    scale, where, received, coeffs_in, basis, res_mix, res, rho, weights, target, coupling,
    out, res_out, rho_out,
):
    at = at_batches(received, damped(scale))
    coeffs = coeffs_in[...]
    slot = where[0]
    sub = iota((HIST, LANES), 0)
    lane = iota((HIST, LANES), 1)
    acc = [jnp.zeros((HIST, LANES), f32)]

    def use(here, density):
        res_new = target[:, here] + coupling[:, here] * jnp.tanh(density) - density
        r = jnp.where(sub == slot, res_new, res[:, here])
        res_out[:, here] = r
        rho_out[:, here] = jnp.where(sub == slot, density, rho[:, here])
        acc[0] = acc[0] + r * (weights[:, here] * res_new)

    density_tiles(at, coeffs, basis, res_mix, rho, use)
    sums = jnp.sum(acc[0], axis=1, keepdims=True)
    row = jnp.sum(jnp.where(lane == sub, sums, 0.0), axis=0, keepdims=True)
    out[...] = jnp.broadcast_to(row, (PEERS, LANES))


def final_kernel(scale, received, coeffs_in, basis, res_mix, rho, density_out, moments_out):
    at = at_batches(received, damped(scale))

    def use(here, density):
        density_out[:, here] = density

    density_tiles(at, coeffs_in[...], basis, res_mix, rho, use)
    for part in range(4):
        rows = pl.ds(16 + 32 * part, 32)
        total = received[0, rows, :]
        for m in range(1, SIDE):
            total = total + received[m, rows, :]
        moments_out[:, pl.ds(part * LANES, LANES)] = (total * scale)[:COMPS]


def local(
    weights,
    target,
    coupling,
    multipole_basis,
    rho_hist,
    res_hist,
    batch_atom,
    owner_slot,
    slot_index,
):
    points = weights.shape[0]
    owned_count = owner_slot.shape[0] // lax.axis_size(ATOM)
    atom_points = points * lax.axis_size(GRID) // owned_count
    scale = 1.0 / math.sqrt(atom_points)
    assert points == POINTS and owned_count == OWNED and multipole_basis.shape[0] == COMPS

    weights, target, coupling = (v.reshape(1, points) for v in (weights, target, coupling))
    slots = owner_slot[batch_atom].astype(f32)
    slots = jnp.concatenate([jnp.zeros((BATCHES,), f32), slots]).reshape(1, LANES)
    place = jnp.stack(
        [lax.axis_index("z"), lax.axis_index("y") * 4 + lax.axis_index("x"), lax.axis_index("c")]
    ).astype(jnp.int32)

    rows = call(gram_kernel, shape(PEERS, LANES), [V, V, V])(res_hist, weights, slots)
    rows = lax.all_to_all(rows, AXES, 0, 0, tiled=True)

    pieces, res_mix, matrix, coeffs = call(
        first_mix_kernel,
        (shape(SIDE, 16, LANES), shape(1, POINTS), shape(HIST, LANES), shape(HIST, LANES)),
        [V, V, V, V],
    )(rows, res_hist, weights, multipole_basis)
    pieces = lax.all_to_all(pieces, COL, 0, 0, tiled=True)
    same, owned = call(
        match_kernel,
        (shape(KNOWN, KNOWN, dtype=bf16), shape(KNOWN, 4 * OWNED, dtype=bf16)),
        [S, V],
        vmem=16 << 20,
    )(place, rows)
    routed = call(route_kernel, shape(SIDE, 16, LANES), [V, V])(pieces, same)
    received = lax.all_to_all(routed, ROW, 0, 0, tiled=True)

    where = slot_index[0:1]
    rows, res_hist, rho_hist = call(
        functools.partial(update_kernel, scale),
        (shape(PEERS, LANES), shape(HIST, POINTS), shape(HIST, POINTS)),
        [S, V, V, V, V, V, V, V, V, V],
    )(where, received, coeffs, multipole_basis, res_mix, res_hist, rho_hist, weights, target, coupling)
    rows = lax.all_to_all(rows, AXES, 0, 0, tiled=True)

    pieces, res_mix, coeffs = call(
        next_mix_kernel,
        (shape(SIDE, 16, LANES), shape(1, POINTS), shape(HIST, LANES)),
        [S, V, V, V, V, V],
    )(where, rows, matrix, res_hist, weights, multipole_basis)
    pieces = lax.all_to_all(pieces, COL, 0, 0, tiled=True)
    routed = call(
        last_route_kernel, shape(SIDE, 16 + 128, LANES), [V, V, V], vmem=20 << 20
    )(pieces, same, owned)
    received = lax.all_to_all(routed, ROW, 0, 0, tiled=True)
    density, moments = call(
        functools.partial(final_kernel, scale), (shape(1, POINTS), shape(COMPS, OWNED)), [V] * 5
    )(received, coeffs, multipole_basis, res_mix, rho_hist)
    return density.reshape(points), moments


def solution(mesh):
    torus = Mesh(mesh.devices.reshape(8, 4, 4, 2), AXES)
    placed = (
        P(AXES),
        P(AXES),
        P(AXES),
        P(None, AXES),
        P(None, AXES),
        P(None, AXES),
        P(AXES),
        P(),
        P(),
    )
    return jax.shard_map(
        local, mesh=torus, in_specs=placed, out_specs=(P(AXES), P(None, ATOM)), check_vma=False
    )
```

```python
import functools
import math

import jax
import jax.numpy as jnp
import numpy as np
from jax import lax
from jax.experimental import pallas as pl
from jax.experimental.pallas import tpu as pltpu
from jax.sharding import Mesh
from jax.sharding import PartitionSpec as P

ITERS = 2
AXES = ("z", "y", "x", "c")
GRID = ("z", "y")
ATOM = ("x", "c")
COL = ("z", "c")
ROW = ("y", "x")

damping_table = np.array(
    [1.0 / (1 + degree) for degree in range(5) for order in range(2 * degree + 1)], dtype=np.float32
)
mixing_beta = 0.5
ridge_share = 0.1

LANES = 128
HIST = 8
COMPS = 25
BATCHES = 64
WIDTH = 256
POINTS = BATCHES * WIDTH
SIDE = 16
DEPTH = 8
KNOWN = SIDE * BATCHES
OWNED = 512
PACKED = 104
NOTE = 100
FINAL = 120

f32 = jnp.float32
bf16 = jnp.bfloat16


def iota(shape, dim):
    return lax.broadcasted_iota(jnp.int32, shape, dim)


def call(kernel, out_shape, in_specs, *, scratch=(), vmem=12 << 20, cost=20000):
    return pl.pallas_call(
        kernel,
        out_shape=out_shape,
        in_specs=[pl.BlockSpec(memory_space=s) for s in in_specs],
        out_specs=jax.tree.map(lambda _: pl.BlockSpec(memory_space=pltpu.VMEM), out_shape),
        scratch_shapes=list(scratch),
        compiler_params=pltpu.CompilerParams(vmem_limit_bytes=vmem),
        cost_estimate=pl.CostEstimate(flops=cost * 1000, bytes_accessed=1 << 20, transcendentals=0),
    )


V = pltpu.VMEM
S = pltpu.SMEM


def shape(*dims, dtype=f32):
    return jax.ShapeDtypeStruct(dims, dtype)


TOPS = (0, 8, 16, 24)
HEIGHTS = (8, 8, 8, 1)


def left_half(rows):
    return iota((rows, LANES), 1) < BATCHES


def swap(value):
    return pltpu.roll(value, BATCHES, 1)


def gram_kernel(res, weights, slots, out):
    acc = [jnp.zeros((HIST, LANES), f32) for _ in range(5)]
    for tile in range(POINTS // LANES):
        at = pl.ds(tile * LANES, LANES)
        r = res[:, at]
        rw = r * weights[:, at]
        acc[0] += rw * r
        for d in range(1, 5):
            acc[d] += rw * pltpu.roll(r, HIST - d, 0)
    lane = iota((HIST, LANES), 1)
    sub = iota((HIST, LANES), 0)
    placed = jnp.zeros((HIST, LANES), f32)
    for d in range(HIST):
        if d < 5:
            sums = jnp.broadcast_to(jnp.sum(acc[d], axis=1, keepdims=True), (HIST, LANES))
        else:
            sums = jnp.broadcast_to(jnp.sum(acc[HIST - d], axis=1, keepdims=True), (HIST, LANES))
            sums = pltpu.roll(sums, HIST - d, 0)
        here = ((lane >> 3) == sub) & ((lane & 7) == ((sub + d) & 7))
        placed = jnp.where(here, sums, placed)
    row = jnp.sum(placed, axis=0, keepdims=True) + slots[...]
    out[...] = jnp.broadcast_to(row, (SIDE, LANES))


def history_moments_kernel(res, weights, basis, out):
    lane = iota((HIST, LANES), 1)
    sub = iota((HIST, LANES), 0)
    for i4 in range(4):
        acc = [jnp.zeros((HEIGHTS[t], LANES), f32) for t in range(4)]
        for b in range(BATCHES):
            for i in (i4, i4 + 4):
                total = [None] * 4
                for half in range(2):
                    at = pl.ds(b * WIDTH + half * LANES, LANES)
                    wr = res[i : i + 1, at] * weights[:, at]
                    for t in range(4):
                        term = basis[pl.ds(TOPS[t], HEIGHTS[t]), at] * wr
                        total[t] = term if half == 0 else total[t] + term
                for t in range(4):
                    sums = jnp.sum(total[t], axis=1, keepdims=True)
                    place = b if i < 4 else b + BATCHES
                    acc[t] = jnp.where(lane[: HEIGHTS[t]] == place, sums, acc[t])
        for t in range(3):
            out[pl.ds(24 * i4 + 8 * t, 8), :] = acc[t]
        out[pl.ds(96 + i4, 1), :] = acc[3]
    out[pl.ds(NOTE, 4), :] = jnp.zeros((4, LANES), f32)


def join_kernel(moments, rows, slots, out):
    note = jnp.sum(rows[...], axis=0, keepdims=True)
    note = jnp.where(left_half(1), note, slots[...])
    for peer in range(DEPTH):
        out[peer, 0:NOTE, :] = moments[0:NOTE, :]
        out[peer, NOTE : NOTE + 1, :] = note
        out[peer, NOTE + 1 : PACKED, :] = moments[NOTE + 1 : PACKED, :]


def solve(matrix):
    lane = iota((HIST, LANES), 1)
    sub = iota((HIST, LANES), 0)
    eye = lane == sub
    trace = jnp.sum(jnp.where(eye, matrix, 0.0), axis=(0, 1), keepdims=True)
    ridge = ridge_share * trace / HIST
    m = jnp.where(eye, matrix + ridge, matrix)
    m = jnp.where(lane == HIST, 1.0, m)
    for j in range(HIST):
        pivot_row = m[j : j + 1, :] / m[j : j + 1, j : j + 1]
        m = jnp.where(sub == j, pivot_row, m - m[:, j : j + 1] * pivot_row)
    z = m[:, HIST : HIST + 1]
    return jnp.broadcast_to(z / jnp.sum(z, axis=0, keepdims=True), (HIST, LANES))


def split3(value):
    hi = value.astype(bf16)
    rest = value - hi.astype(f32)
    mid = rest.astype(bf16)
    lo = (rest - mid.astype(f32)).astype(bf16)
    return jnp.concatenate([hi, mid, lo], axis=0)


def add_terms(product):
    return product[0:32] + product[32:64] + product[64:96]


def first_row(value):
    return jnp.where(iota((8, LANES), 0) == 0, jnp.broadcast_to(value, (8, LANES)), 0.0)


def mixed_history(coeffs, own, other):
    left = left_half(1)
    c = [jnp.where(left, coeffs[i : i + 1], coeffs[i + 4 : i + 5]) for i in range(4)]
    tiles = []
    for z in range(DEPTH):
        halves = []
        for side in (own, other):
            body = sum(side[z, 24 * i : 24 * i + 24, :] * c[i] for i in range(4))
            last = sum(side[z, 96 + i : 97 + i, :] * c[i] for i in range(4))
            halves.append((body + swap(body), last + swap(last)))
        body = jnp.where(left_half(24), halves[0][0], halves[1][0])
        last = jnp.where(left, halves[0][1], halves[1][1])
        tiles.append(jnp.concatenate([body, first_row(last)], axis=0))
    return tiles


def known_slots(own, other):
    rows = [side[z, NOTE : NOTE + 1, :] for z in range(DEPTH) for side in (own, other)]
    down = jnp.transpose(jnp.concatenate(rows, axis=0))[LANES - BATCHES :, :]
    left = left_half(1)
    along = [jnp.where(left, swap(rows[2 * z]), rows[2 * z + 1]) for z in range(DEPTH)]
    return down, along


def to_targets(sums, out):
    left = left_half(16)
    for q in range(SIDE // 2):
        low = sums[0:16, q * LANES : (q + 1) * LANES]
        high = sums[16:32, q * LANES : (q + 1) * LANES]
        out[2 * q, 0:16, :] = jnp.where(left, low, swap(high))
        out[2 * q + 1, 0:16, :] = jnp.where(left, swap(low), high)


def first_route_kernel(own, other, rows, out, same, matrix_out, coeffs_out):
    note = own[0, NOTE : NOTE + 1, :] + other[0, NOTE : NOTE + 1, :]
    for z in range(1, DEPTH):
        note = note + own[z, NOTE : NOTE + 1, :] + other[z, NOTE : NOTE + 1, :]
    wide = jnp.broadcast_to(note, (HIST, LANES))
    sub = iota((HIST, LANES), 0)
    matrix = wide
    for i in range(1, HIST):
        matrix = jnp.where(sub == i, pltpu.roll(wide, LANES - HIST * i, 1), matrix)
    matrix = jnp.where(iota((HIST, LANES), 1) < HIST, matrix, 0.0)
    matrix_out[...] = matrix
    coeffs = solve(matrix)
    coeffs_out[...] = coeffs

    down, _ = known_slots(own, other)
    left = left_half(1)
    wanted = [
        jnp.where(left, swap(rows[2 * q : 2 * q + 1, :]), rows[2 * q + 1 : 2 * q + 2, :])
        for q in range(SIDE // 2)
    ]
    for i in range(SIDE):
        mine = jnp.broadcast_to(down[:, i : i + 1], (BATCHES, LANES))
        for q in range(SIDE // 2):
            hit = jnp.where(mine == wanted[q], 1.0, 0.0)
            same[pl.ds(i * BATCHES, BATCHES), pl.ds(q * LANES, LANES)] = hit.astype(bf16)

    terms = split3(jnp.concatenate(mixed_history(coeffs, own, other), axis=1))
    to_targets(add_terms(jnp.dot(terms, same[...], preferred_element_type=f32)), out)


def row_sum_kernel(pieces, out):
    row = pieces[0, 15:16, :]
    for m in range(1, SIDE):
        row = row + pieces[m, 15:16, :]
    out[...] = jnp.broadcast_to(row, (SIDE, LANES))


def last_route_kernel(
    where, place, rows, matrix_in, own, other, pieces, same, out, coeffs_out, low_hot
):
    slot, c0 = where[0], place[0]
    row = swap(jnp.sum(rows[...], axis=0, keepdims=True))
    row = jnp.broadcast_to(row, (HIST, LANES))
    lane = iota((HIST, LANES), 1)
    sub = iota((HIST, LANES), 0)
    column = jnp.sum(jnp.where(lane == sub, row, 0.0), axis=1, keepdims=True)
    matrix = jnp.where(sub == slot, row, jnp.where(lane == slot, column, matrix_in[...]))
    matrix = jnp.where(lane < HIST, matrix, 0.0)
    coeffs = solve(matrix)
    coeffs_out[...] = coeffs
    fresh = jnp.sum(jnp.where(sub == slot, coeffs, 0.0), axis=0, keepdims=True)

    tiles = mixed_history(jnp.where(sub == slot, 0.0, coeffs), own, other)
    left = left_half(16)
    for z in range(DEPTH):
        a = jnp.where(c0 == 0, pieces[2 * z], pieces[2 * z + 1])
        b = jnp.where(c0 == 0, pieces[2 * z + 1], pieces[2 * z])
        low = jnp.where(left, a, swap(b))
        high = jnp.where(left, swap(a), b)
        new = jnp.concatenate([low, high[0:8], first_row(high[8:9])], axis=0)
        tiles[z] = tiles[z] + fresh * new
    terms = split3(jnp.concatenate(tiles, axis=1))
    to_targets(add_terms(jnp.dot(terms, same[...], preferred_element_type=f32)), out)

    down, along = known_slots(own, other)
    low_bits = down.astype(jnp.int32) & 255
    for i in range(SIDE):
        mine = jnp.broadcast_to(low_bits[:, i : i + 1], (BATCHES, LANES))
        for half in range(2):
            hit = jnp.where(mine == iota((BATCHES, LANES), 1) + half * LANES, 1.0, 0.0)
            low_hot[pl.ds(i * BATCHES, BATCHES), pl.ds(half * LANES, LANES)] = hit.astype(bf16)
    high_bits = jnp.concatenate(along, axis=1).astype(jnp.int32) >> 8
    masked = []
    for x in range(4):
        for half in range(2):
            pick = jnp.where(high_bits == (2 * x + c0) * 2 + half, 1.0, 0.0)
            pick = jnp.broadcast_to(pick, (96, KNOWN)).astype(bf16)
            masked.append(terms * pick)
    product = jnp.dot(
        jnp.concatenate(masked, axis=0), low_hot[...], preferred_element_type=f32
    )
    for x in range(4):
        ends = jnp.zeros((8, LANES), f32)
        for part in range(4):
            at = 96 * (2 * x + part // 2)
            sums = add_terms(product[at : at + 96, (part % 2) * LANES : (part % 2 + 1) * LANES])
            ends = jnp.where(sub == part, jnp.broadcast_to(sums[24:25], (8, LANES)), ends)
            for y in range(4):
                out[4 * y + x, pl.ds(16 + 24 * part, 24), :] = sums[0:24]
        for y in range(4):
            out[4 * y + x, pl.ds(112, 8), :] = ends


def at_batches(received, scales):
    total = received[0, 0:16, :]
    for m in range(1, SIDE):
        total = total + received[m, 0:16, :]
    return jnp.concatenate([total, swap(total)], axis=0) * scales


def damped(scale):
    k = iota((32, LANES), 0)
    value = jnp.full((32, LANES), float(damping_table[0]), f32)
    for degree in range(1, 5):
        value = jnp.where(k >= degree * degree, float(np.float32(1.0 / (1 + degree))), value)
    return jnp.where(k < COMPS, value * scale, 0.0)


def correction(at, b):
    return [
        jnp.broadcast_to(at[TOPS[t] : TOPS[t] + HEIGHTS[t], b : b + 1], (HEIGHTS[t], LANES))
        for t in range(4)
    ]


def correct_tile(wide, basis):
    terms = sum(wide[t] * basis[t] for t in range(3))
    return jnp.sum(terms, axis=0, keepdims=True) + wide[3] * basis[3]


def update_kernel(
    scale, where, received, coeffs_in, basis, res, rho, weights, target, coupling, out, mixed_out
):
    at = at_batches(received, damped(scale))
    coeffs = coeffs_in[...]
    slot = where[0]
    sub = iota((HIST, LANES), 0)
    lane = iota((HIST, LANES), 1)
    overlap = jnp.zeros((HIST, LANES), f32)
    acc = [jnp.zeros((h, LANES), f32) for h in HEIGHTS]
    for b in range(BATCHES):
        wide = correction(at, b)
        total = [None] * 4
        for half in range(2):
            here = pl.ds(b * WIDTH + half * LANES, LANES)
            y = [basis[pl.ds(TOPS[t], HEIGHTS[t]), here] for t in range(4)]
            r = res[:, here]
            mixed = rho[:, here] + mixing_beta * r
            density = jnp.sum(coeffs * mixed, axis=0, keepdims=True)
            density = density - mixing_beta * correct_tile(wide, y)
            res_new = target[:, here] + coupling[:, here] * jnp.tanh(density) - density
            mixed_out[:, here] = jnp.where(sub == slot, density + mixing_beta * res_new, mixed)
            wr = weights[:, here] * res_new
            overlap = overlap + jnp.where(sub == slot, res_new, r) * wr
            for t in range(4):
                total[t] = y[t] * wr if half == 0 else total[t] + y[t] * wr
        for t in range(4):
            sums = jnp.sum(total[t], axis=1, keepdims=True)
            place = b if t < 2 else b + BATCHES
            acc[t] = jnp.where(lane[: HEIGHTS[t]] == place, sums, acc[t])
    sums = jnp.sum(overlap, axis=1, keepdims=True)
    row = jnp.sum(jnp.where(lane == sub + BATCHES, sums, 0.0), axis=0, keepdims=True)
    row = jnp.broadcast_to(row, (8, LANES))
    end = jnp.where(sub == 7, row, first_row(acc[3]))
    packed = jnp.concatenate([acc[0] + acc[2], acc[1] + end], axis=0)
    for peer in range(SIDE):
        out[peer] = packed


def final_kernel(scale, received, coeffs_in, basis, mixed, density_out, moments_out):
    at = at_batches(received, damped(scale))
    coeffs = coeffs_in[...]
    for b in range(BATCHES):
        wide = correction(at, b)
        for half in range(2):
            here = pl.ds(b * WIDTH + half * LANES, LANES)
            y = [basis[pl.ds(TOPS[t], HEIGHTS[t]), here] for t in range(4)]
            density = jnp.sum(coeffs * mixed[:, here], axis=0, keepdims=True)
            density_out[:, here] = density - mixing_beta * correct_tile(wide, y)
    total = received[0, 16:FINAL, :]
    for m in range(1, SIDE):
        total = total + received[m, 16:FINAL, :]
    total = total * scale
    for part in range(4):
        at = pl.ds(part * LANES, LANES)
        moments_out[0:24, at] = total[24 * part : 24 * part + 24]
        moments_out[24:25, at] = total[96 + part : 97 + part]


def exchange(pieces, axes):
    return lax.all_to_all(pieces, axes, 0, 0, tiled=True)


def local(
    weights,
    target,
    coupling,
    multipole_basis,
    rho_hist,
    res_hist,
    batch_atom,
    owner_slot,
    slot_index,
):
    points = weights.shape[0]
    owned_count = owner_slot.shape[0] // lax.axis_size(ATOM)
    atom_points = points * lax.axis_size(GRID) // owned_count
    scale = 1.0 / math.sqrt(atom_points)
    assert points == POINTS and owned_count == OWNED and multipole_basis.shape[0] == COMPS

    weights, target, coupling = (v.reshape(1, points) for v in (weights, target, coupling))
    slots = owner_slot[batch_atom].astype(f32)
    slots = jnp.concatenate([jnp.zeros((BATCHES,), f32), slots]).reshape(1, LANES)
    where = slot_index[0:1]
    place = lax.axis_index("c").astype(jnp.int32).reshape(1)

    rows = call(gram_kernel, shape(SIDE, LANES), [V] * 3)(res_hist, weights, slots)
    rows = exchange(rows, ROW)
    history = call(history_moments_kernel, shape(PACKED, LANES), [V] * 3)(
        res_hist, weights, multipole_basis
    )
    own = call(join_kernel, shape(DEPTH, PACKED, LANES), [V] * 3)(history, rows, slots)
    own = exchange(own, ("z",))
    other = lax.ppermute(own, "c", [(0, 1), (1, 0)])
    pieces, same, matrix, coeffs = call(
        first_route_kernel,
        (
            shape(SIDE, 16, LANES),
            shape(KNOWN, KNOWN, dtype=bf16),
            shape(HIST, LANES),
            shape(HIST, LANES),
        ),
        [V] * 3,
    )(own, other, rows)
    received = exchange(pieces, ROW)

    pieces, mixed = call(
        functools.partial(update_kernel, scale),
        (shape(SIDE, 16, LANES), shape(HIST, POINTS)),
        [S] + [V] * 8,
    )(where, received, coeffs, multipole_basis, res_hist, rho_hist, weights, target, coupling)
    pieces = exchange(pieces, COL)
    rows = call(row_sum_kernel, shape(SIDE, LANES), [V])(pieces)
    rows = exchange(rows, ROW)
    routed, coeffs = call(
        last_route_kernel,
        (shape(SIDE, FINAL, LANES), shape(HIST, LANES)),
        [S, S] + [V] * 6,
        scratch=[pltpu.VMEM((KNOWN, 256), bf16)],
        vmem=20 << 20,
    )(where, place, rows, matrix, own, other, pieces, same)
    received = exchange(routed, ROW)
    density, moments = call(
        functools.partial(final_kernel, scale), (shape(1, POINTS), shape(COMPS, OWNED)), [V] * 4
    )(received, coeffs, multipole_basis, mixed)
    return density.reshape(points), moments


def solution(mesh):
    torus = Mesh(mesh.devices.reshape(8, 4, 4, 2), AXES)
    placed = (
        P(AXES),
        P(AXES),
        P(AXES),
        P(None, AXES),
        P(None, AXES),
        P(None, AXES),
        P(AXES),
        P(),
        P(),
    )
    return jax.shard_map(
        local, mesh=torus, in_specs=placed, out_specs=(P(AXES), P(None, ATOM)), check_vma=False
    )
```

```python
import functools
import math

import jax
import jax.numpy as jnp
import numpy as np
from jax import lax
from jax.experimental import pallas as pl
from jax.experimental.pallas import tpu as pltpu
from jax.sharding import Mesh
from jax.sharding import PartitionSpec as P

ITERS = 2
AXES = ("z", "y", "x", "c")
GRID = ("z", "y")
ATOM = ("x", "c")
COL = ("z", "c")
ROW = ("y", "x")

damping_table = np.array(
    [1.0 / (1 + degree) for degree in range(5) for order in range(2 * degree + 1)], dtype=np.float32
)
mixing_beta = 0.5
ridge_share = 0.1

LANES = 128
HIST = 8
COMPS = 25
BATCHES = 64
WIDTH = 256
POINTS = BATCHES * WIDTH
SIDE = 16
KNOWN = SIDE * BATCHES
OWNED = 512
PACKED = 104
NOTE = 100
FINAL = 40
QUARTER = OWNED // 4

f32 = jnp.float32
bf16 = jnp.bfloat16


def iota(shape, dim):
    return lax.broadcasted_iota(jnp.int32, shape, dim)


def call(kernel, out_shape, in_specs, *, scratch=(), vmem=12 << 20, cost=20000):
    return pl.pallas_call(
        kernel,
        out_shape=out_shape,
        in_specs=[pl.BlockSpec(memory_space=s) for s in in_specs],
        out_specs=jax.tree.map(lambda _: pl.BlockSpec(memory_space=pltpu.VMEM), out_shape),
        scratch_shapes=list(scratch),
        compiler_params=pltpu.CompilerParams(vmem_limit_bytes=vmem),
        cost_estimate=pl.CostEstimate(flops=cost * 1000, bytes_accessed=1 << 20, transcendentals=0),
    )


V = pltpu.VMEM
S = pltpu.SMEM


def shape(*dims, dtype=f32):
    return jax.ShapeDtypeStruct(dims, dtype)


TOPS = (0, 8, 16, 24)
HEIGHTS = (8, 8, 8, 1)


def left_half(rows):
    return iota((rows, LANES), 1) < BATCHES


def swap(value):
    return pltpu.roll(value, BATCHES, 1)


def slots_of(atoms, table):
    hits = jnp.where(iota((32, BATCHES), 0) == (atoms >> 7), 1.0, 0.0).astype(bf16)
    halves = []
    for half in (table >> 6, table & 63):
        rows = lax.dot_general(
            half.astype(f32).astype(bf16), hits, (((0,), (0,)), ((), ())),
            preferred_element_type=f32,
        )
        mine = iota((LANES, BATCHES), 0) == (atoms & 127)
        halves.append(jnp.sum(jnp.where(mine, rows, 0.0), axis=0, keepdims=True))
    return halves[0] * 64.0 + halves[1]


def gram_kernel(res, weights, atoms, table, out):
    acc = [jnp.zeros((HIST, LANES), f32) for _ in range(5)]
    for tile in range(POINTS // LANES):
        at = pl.ds(tile * LANES, LANES)
        r = res[:, at]
        rw = r * weights[:, at]
        acc[0] += rw * r
        for d in range(1, 5):
            acc[d] += rw * pltpu.roll(r, HIST - d, 0)
    lane = iota((HIST, LANES), 1)
    sub = iota((HIST, LANES), 0)
    placed = jnp.zeros((HIST, LANES), f32)
    for d in range(HIST):
        if d < 5:
            sums = jnp.broadcast_to(jnp.sum(acc[d], axis=1, keepdims=True), (HIST, LANES))
        else:
            sums = jnp.broadcast_to(jnp.sum(acc[HIST - d], axis=1, keepdims=True), (HIST, LANES))
            sums = pltpu.roll(sums, HIST - d, 0)
        here = ((lane >> 3) == sub) & ((lane & 7) == ((sub + d) & 7))
        placed = jnp.where(here, sums, placed)
    slots = slots_of(atoms[...], table[...])
    slots = jnp.concatenate([jnp.zeros((1, BATCHES), f32), slots], axis=1)
    row = jnp.sum(placed, axis=0, keepdims=True) + slots
    out[...] = jnp.broadcast_to(row, (SIDE, LANES))


def history_moments_kernel(res, weights, basis, sent, rows, out):
    lane = iota((HIST, LANES), 1)
    for i4 in range(4):
        acc = [jnp.zeros((HEIGHTS[t], LANES), f32) for t in range(4)]
        for b in range(BATCHES):
            for i in (i4, i4 + 4):
                total = [None] * 4
                for half in range(2):
                    at = pl.ds(b * WIDTH + half * LANES, LANES)
                    wr = res[i : i + 1, at] * weights[:, at]
                    for t in range(4):
                        term = basis[pl.ds(TOPS[t], HEIGHTS[t]), at] * wr
                        total[t] = term if half == 0 else total[t] + term
                for t in range(4):
                    sums = jnp.sum(total[t], axis=1, keepdims=True)
                    place = b if i < 4 else b + BATCHES
                    acc[t] = jnp.where(lane[: HEIGHTS[t]] == place, sums, acc[t])
        for peer in range(SIDE):
            for t in range(3):
                out[peer, pl.ds(24 * i4 + 8 * t, 8), :] = acc[t]
            out[peer, pl.ds(96 + i4, 1), :] = acc[3]
    note = jnp.sum(rows[...], axis=0, keepdims=True)
    note = first_row(jnp.where(left_half(1), note, sent[0:1, :]))
    for peer in range(SIDE):
        out[peer, pl.ds(NOTE, 4), :] = note[0:4]


def solve(matrix):
    lane = iota((HIST, LANES), 1)
    sub = iota((HIST, LANES), 0)
    eye = lane == sub
    trace = jnp.sum(jnp.where(eye, matrix, 0.0), axis=(0, 1), keepdims=True)
    ridge = ridge_share * trace / HIST
    m = jnp.where(eye, matrix + ridge, matrix)
    m = jnp.where(lane == HIST, 1.0, m)
    for j in range(HIST):
        pivot_row = m[j : j + 1, :] / m[j : j + 1, j : j + 1]
        m = jnp.where(sub == j, pivot_row, m - m[:, j : j + 1] * pivot_row)
    z = m[:, HIST : HIST + 1]
    return jnp.broadcast_to(z / jnp.sum(z, axis=0, keepdims=True), (HIST, LANES))


def split3(value):
    hi = value.astype(bf16)
    rest = value - hi.astype(f32)
    mid = rest.astype(bf16)
    lo = (rest - mid.astype(f32)).astype(bf16)
    return jnp.concatenate([hi, mid, lo], axis=0)


def add_terms(product):
    return product[0:32] + product[32:64] + product[64:96]


def first_row(value):
    return jnp.where(iota((8, LANES), 0) == 0, jnp.broadcast_to(value, (8, LANES)), 0.0)


def mixed_history(coeffs, history):
    left = left_half(1)
    c = [jnp.where(left, coeffs[i : i + 1], coeffs[i + 4 : i + 5]) for i in range(4)]
    tiles = []
    for q in range(SIDE // 2):
        halves = []
        for m in (2 * q, 2 * q + 1):
            body = sum(history[m, 24 * i : 24 * i + 24, :] * c[i] for i in range(4))
            last = sum(history[m, 96 + i : 97 + i, :] * c[i] for i in range(4))
            halves.append((body + swap(body), last + swap(last)))
        body = jnp.where(left_half(24), halves[0][0], halves[1][0])
        last = jnp.where(left, halves[0][1], halves[1][1])
        tiles.append(jnp.concatenate([body, first_row(last)], axis=0))
    return tiles


def in_pairs(rows):
    left = left_half(1)
    return [jnp.where(left, swap(rows[2 * q]), rows[2 * q + 1]) for q in range(SIDE // 2)]


def known_slots(history):
    rows = [history[m, NOTE : NOTE + 1, :] for m in range(SIDE)]
    down = jnp.transpose(jnp.concatenate(rows, axis=0))[LANES - BATCHES :, :]
    return down, in_pairs(rows)


def to_targets(sums, out):
    left = left_half(16)
    for q in range(SIDE // 2):
        low = sums[0:16, q * LANES : (q + 1) * LANES]
        high = sums[16:32, q * LANES : (q + 1) * LANES]
        out[2 * q, 0:16, :] = jnp.where(left, low, swap(high))
        out[2 * q + 1, 0:16, :] = jnp.where(left, swap(low), high)


def first_route_kernel(history, rows, out, same, matrix_out, coeffs_out):
    note = history[0, NOTE : NOTE + 1, :]
    for m in range(1, SIDE):
        note = note + history[m, NOTE : NOTE + 1, :]
    wide = jnp.broadcast_to(note, (HIST, LANES))
    sub = iota((HIST, LANES), 0)
    matrix = wide
    for i in range(1, HIST):
        matrix = jnp.where(sub == i, pltpu.roll(wide, LANES - HIST * i, 1), matrix)
    matrix = jnp.where(iota((HIST, LANES), 1) < HIST, matrix, 0.0)
    matrix_out[...] = matrix
    coeffs = solve(matrix)
    coeffs_out[...] = coeffs

    down, _ = known_slots(history)
    wanted = in_pairs([rows[m : m + 1, :] for m in range(SIDE)])
    for i in range(SIDE):
        mine = jnp.broadcast_to(down[:, i : i + 1], (BATCHES, LANES))
        for q in range(SIDE // 2):
            hit = jnp.where(mine == wanted[q], 1.0, 0.0)
            same[pl.ds(i * BATCHES, BATCHES), pl.ds(q * LANES, LANES)] = hit.astype(bf16)

    terms = split3(jnp.concatenate(mixed_history(coeffs, history), axis=1))
    to_targets(add_terms(jnp.dot(terms, same[...], preferred_element_type=f32)), out)


def row_sum_kernel(pieces, out):
    row = pieces[0, 15:16, :]
    for m in range(1, SIDE):
        row = row + pieces[m, 15:16, :]
    out[...] = jnp.broadcast_to(row, (SIDE, LANES))


def last_route_kernel(
    where, place, rows, matrix_in, history, pieces, same, out, coeffs_out, low_hot
):
    slot, first = where[0], place[0]
    row = swap(jnp.sum(rows[...], axis=0, keepdims=True))
    row = jnp.broadcast_to(row, (HIST, LANES))
    lane = iota((HIST, LANES), 1)
    sub = iota((HIST, LANES), 0)
    column = jnp.sum(jnp.where(lane == sub, row, 0.0), axis=1, keepdims=True)
    matrix = jnp.where(sub == slot, row, jnp.where(lane == slot, column, matrix_in[...]))
    matrix = jnp.where(lane < HIST, matrix, 0.0)
    coeffs = solve(matrix)
    coeffs_out[...] = coeffs
    fresh = jnp.sum(jnp.where(sub == slot, coeffs, 0.0), axis=0, keepdims=True)

    tiles = mixed_history(jnp.where(sub == slot, 0.0, coeffs), history)
    left = left_half(16)
    for q in range(SIDE // 2):
        a, b = pieces[2 * q], pieces[2 * q + 1]
        low = jnp.where(left, a, swap(b))
        high = jnp.where(left, swap(a), b)
        new = jnp.concatenate([low, high[0:8], first_row(high[8:9])], axis=0)
        tiles[q] = tiles[q] + fresh * new
    terms = split3(jnp.concatenate(tiles, axis=1))
    to_targets(add_terms(jnp.dot(terms, same[...], preferred_element_type=f32)), out)

    down, along = known_slots(history)
    low_bits = down.astype(jnp.int32) & 127
    for i in range(SIDE):
        mine = jnp.broadcast_to(low_bits[:, i : i + 1], (BATCHES, LANES))
        hit = jnp.where(mine == iota((BATCHES, LANES), 1), 1.0, 0.0)
        low_hot[pl.ds(i * BATCHES, BATCHES), :] = hit.astype(bf16)
    high_bits = jnp.concatenate(along, axis=1).astype(jnp.int32) >> 7
    masked = []
    for c in range(2):
        pick = jnp.where(high_bits == first + 4 * c, 1.0, 0.0)
        masked.append(terms * jnp.broadcast_to(pick, (96, KNOWN)).astype(bf16))
    product = jnp.dot(
        jnp.concatenate(masked, axis=0), low_hot[...], preferred_element_type=f32
    )
    left = left_half(1)
    for c in range(2):
        sums = add_terms(product[96 * c : 96 * c + 96])
        end = sums[24:25]
        for z in range(SIDE // 2):
            m = 2 * z + c
            out[m, 16:FINAL, :] = sums[0:24]
            out[m, 9:10, :] = jnp.where(left, out[m, 9:10, :], swap(end))
            out[m, 10:11, :] = jnp.where(left, out[m, 10:11, :], end)


def at_batches(received, scales):
    total = received[0, 0:16, :]
    for m in range(1, SIDE):
        total = total + received[m, 0:16, :]
    return jnp.concatenate([total, swap(total)], axis=0) * scales


def damped(scale):
    k = iota((32, LANES), 0)
    value = jnp.full((32, LANES), float(damping_table[0]), f32)
    for degree in range(1, 5):
        value = jnp.where(k >= degree * degree, float(np.float32(1.0 / (1 + degree))), value)
    return jnp.where(k < COMPS, value * scale, 0.0)


def correction(at, b):
    return [
        jnp.broadcast_to(at[TOPS[t] : TOPS[t] + HEIGHTS[t], b : b + 1], (HEIGHTS[t], LANES))
        for t in range(4)
    ]


def correct_tile(wide, basis):
    terms = sum(wide[t] * basis[t] for t in range(3))
    return jnp.sum(terms, axis=0, keepdims=True) + wide[3] * basis[3]


def basis_tiles(basis, here):
    return [basis[pl.ds(TOPS[t], HEIGHTS[t]), here] for t in range(4)]


def update_kernel(
    scale, where, received, coeffs_in, basis, res, rho, weights, target, coupling,
    out, mixed_out, weighted,
):
    at = at_batches(received, damped(scale))
    coeffs = coeffs_in[...]
    slot = where[0]
    sub = iota((HIST, LANES), 0)
    lane = iota((HIST, LANES), 1)
    overlap = jnp.zeros((HIST, LANES), f32)
    for b in range(BATCHES):
        wide = correction(at, b)
        for half in range(2):
            here = pl.ds(b * WIDTH + half * LANES, LANES)
            r = res[:, here]
            mixed = rho[:, here] + mixing_beta * r
            density = jnp.sum(coeffs * mixed, axis=0, keepdims=True)
            density = density - mixing_beta * correct_tile(wide, basis_tiles(basis, here))
            res_new = target[:, here] + coupling[:, here] * jnp.tanh(density) - density
            mixed_out[:, here] = jnp.where(sub == slot, density + mixing_beta * res_new, mixed)
            wr = weights[:, here] * res_new
            weighted[:, here] = wr
            overlap = overlap + jnp.where(sub == slot, res_new, r) * wr
    acc = [jnp.zeros((h, LANES), f32) for h in HEIGHTS]
    for b in range(BATCHES):
        total = [None] * 4
        for half in range(2):
            here = pl.ds(b * WIDTH + half * LANES, LANES)
            wr = weighted[:, here]
            y = basis_tiles(basis, here)
            for t in range(4):
                total[t] = y[t] * wr if half == 0 else total[t] + y[t] * wr
        for t in range(4):
            sums = jnp.sum(total[t], axis=1, keepdims=True)
            place = b if t < 2 else b + BATCHES
            acc[t] = jnp.where(lane[: HEIGHTS[t]] == place, sums, acc[t])
    sums = jnp.sum(overlap, axis=1, keepdims=True)
    row = jnp.sum(jnp.where(lane == sub + BATCHES, sums, 0.0), axis=0, keepdims=True)
    row = jnp.broadcast_to(row, (8, LANES))
    end = jnp.where(sub == 7, row, first_row(acc[3]))
    packed = jnp.concatenate([acc[0] + acc[2], acc[1] + end], axis=0)
    for peer in range(SIDE):
        out[peer] = packed


def quarter_kernel(scale, received, out):
    total = received[0]
    for m in range(1, SIDE):
        total = total + received[m]
    total = total * scale
    end = jnp.where(left_half(1), swap(total[9:10]), total[10:11])
    for y in range(4):
        out[y, 0:24, :] = total[16:FINAL]
        out[y, 24:32, :] = first_row(end)


def final_kernel(scale, received, coeffs_in, basis, mixed, quarters, density_out, moments_out):
    at = at_batches(received, damped(scale))
    coeffs = coeffs_in[...]
    for b in range(BATCHES):
        wide = correction(at, b)
        for half in range(2):
            here = pl.ds(b * WIDTH + half * LANES, LANES)
            density = jnp.sum(coeffs * mixed[:, here], axis=0, keepdims=True)
            correct = correct_tile(wide, basis_tiles(basis, here))
            density_out[:, here] = density - mixing_beta * correct
    for y in range(4):
        moments_out[:, pl.ds(y * QUARTER, QUARTER)] = quarters[y, 0:COMPS, :]


def exchange(pieces, axes):
    return lax.all_to_all(pieces, axes, 0, 0, tiled=True)


def local(
    weights,
    target,
    coupling,
    multipole_basis,
    rho_hist,
    res_hist,
    batch_atom,
    owner_slot,
    slot_index,
):
    points = weights.shape[0]
    owned_count = owner_slot.shape[0] // lax.axis_size(ATOM)
    atom_points = points * lax.axis_size(GRID) // owned_count
    scale = 1.0 / math.sqrt(atom_points)
    assert points == POINTS and owned_count == OWNED and multipole_basis.shape[0] == COMPS

    weights, target, coupling = (v.reshape(1, points) for v in (weights, target, coupling))
    atoms = batch_atom.reshape(1, BATCHES)
    table = owner_slot.reshape(-1, LANES)
    place = (lax.axis_index("x") * 8 + lax.axis_index("y")).astype(jnp.int32).reshape(1)
    atoms, place, where = lax.optimization_barrier((atoms, place, slot_index[0:1]))

    sent = call(gram_kernel, shape(SIDE, LANES), [V] * 4)(res_hist, weights, atoms, table)
    rows = exchange(sent, COL)
    history = call(history_moments_kernel, shape(SIDE, PACKED, LANES), [V] * 5)(
        res_hist, weights, multipole_basis, sent, rows
    )
    history = exchange(history, ROW)
    pieces, same, matrix, coeffs = call(
        first_route_kernel,
        (
            shape(SIDE, 16, LANES),
            shape(KNOWN, KNOWN, dtype=bf16),
            shape(HIST, LANES),
            shape(HIST, LANES),
        ),
        [V] * 2,
    )(history, rows)
    received = exchange(pieces, COL)

    pieces, mixed = call(
        functools.partial(update_kernel, scale),
        (shape(SIDE, 16, LANES), shape(HIST, POINTS)),
        [S] + [V] * 8,
        scratch=[pltpu.VMEM((1, POINTS), f32)],
    )(where, received, coeffs, multipole_basis, res_hist, rho_hist, weights, target, coupling)
    pieces = exchange(pieces, ROW)
    rows = call(row_sum_kernel, shape(SIDE, LANES), [V])(pieces)
    rows = exchange(rows, COL)
    routed, coeffs = call(
        last_route_kernel,
        (shape(SIDE, FINAL, LANES), shape(HIST, LANES)),
        [S, S] + [V] * 5,
        scratch=[pltpu.VMEM((KNOWN, LANES), bf16)],
    )(where, place, rows, matrix, history, pieces, same)
    received = exchange(routed, COL)
    quarters = call(functools.partial(quarter_kernel, scale), shape(4, 32, LANES), [V])(received)
    quarters = exchange(quarters, ("y",))
    density, moments = call(
        functools.partial(final_kernel, scale), (shape(1, POINTS), shape(COMPS, OWNED)), [V] * 5
    )(received, coeffs, multipole_basis, mixed, quarters)
    return density.reshape(points), moments


def solution(mesh):
    torus = Mesh(mesh.devices.reshape(8, 4, 4, 2), AXES)
    placed = (
        P(AXES),
        P(AXES),
        P(AXES),
        P(None, AXES),
        P(None, AXES),
        P(None, AXES),
        P(AXES),
        P(),
        P(),
    )
    return jax.shard_map(
        local, mesh=torus, in_specs=placed, out_specs=(P(AXES), P(None, ATOM)), check_vma=False
    )
```

```python
import functools
import math

import jax
import jax.numpy as jnp
import numpy as np
from jax import lax
from jax.experimental import pallas as pl
from jax.experimental.pallas import tpu as pltpu
from jax.sharding import Mesh
from jax.sharding import PartitionSpec as P

ITERS = 2
AXES = ("z", "y", "x", "c")
GRID = ("z", "y")
ATOM = ("x", "c")
COL = ("z", "c")
ROW = ("y", "x")

damping_table = np.array(
    [1.0 / (1 + degree) for degree in range(5) for order in range(2 * degree + 1)], dtype=np.float32
)
mixing_beta = 0.5
ridge_share = 0.1

LANES = 128
HIST = 8
COMPS = 25
BATCHES = 64
WIDTH = 256
POINTS = BATCHES * WIDTH
SIDE = 16
KNOWN = SIDE * BATCHES
OWNED = 512
PACKED = 104
NOTE = 100
FINAL = 40
QUARTER = OWNED // 4
PARTS = 4

f32 = jnp.float32
bf16 = jnp.bfloat16


def iota(shape, dim):
    return lax.broadcasted_iota(jnp.int32, shape, dim)


def call(kernel, out_shape, in_specs, *, scratch=(), vmem=12 << 20, cost=20000):
    return pl.pallas_call(
        kernel,
        out_shape=out_shape,
        in_specs=[pl.BlockSpec(memory_space=s) for s in in_specs],
        out_specs=jax.tree.map(lambda _: pl.BlockSpec(memory_space=pltpu.VMEM), out_shape),
        scratch_shapes=list(scratch),
        compiler_params=pltpu.CompilerParams(vmem_limit_bytes=vmem),
        cost_estimate=pl.CostEstimate(flops=cost * 1000, bytes_accessed=1 << 20, transcendentals=0),
    )


V = pltpu.VMEM
S = pltpu.SMEM


def shape(*dims, dtype=f32):
    return jax.ShapeDtypeStruct(dims, dtype)


TOPS = (0, 8, 16, 24)
HEIGHTS = (8, 8, 8, 1)


def left_half(rows):
    return iota((rows, LANES), 1) < BATCHES


def swap(value):
    return pltpu.roll(value, BATCHES, 1)


def slots_of(atoms, table):
    hits = jnp.where(iota((32, BATCHES), 0) == (atoms >> 7), 1.0, 0.0).astype(bf16)
    halves = []
    for half in (table >> 6, table & 63):
        rows = lax.dot_general(
            half.astype(f32).astype(bf16), hits, (((0,), (0,)), ((), ())),
            preferred_element_type=f32,
        )
        mine = iota((LANES, BATCHES), 0) == (atoms & 127)
        halves.append(jnp.sum(jnp.where(mine, rows, 0.0), axis=0, keepdims=True))
    return halves[0] * 64.0 + halves[1]


def gram_kernel(
    res_in, weights_in, atoms_in, table_in, basis_in,
    out, res, weights, basis,
    atoms, table, sems,
):
    def fetch(source, target, sem):
        copy = pltpu.make_async_copy(source, target, sems.at[sem])
        copy.start()
        return copy

    step = POINTS // PARTS
    fetches = [fetch(weights_in, weights, 0)]
    for part in range(PARTS):
        at = (slice(None), pl.ds(part * step, step))
        fetches.append(fetch(res_in.at[at], res.at[at], 1 + part))
    small = [fetch(atoms_in, atoms, 1 + PARTS), fetch(table_in, table, 2 + PARTS)]
    last = fetch(basis_in, basis, 3 + PARTS)

    acc = [jnp.zeros((HIST, LANES), f32) for _ in range(5)]
    fetches[0].wait()
    for part in range(PARTS):
        fetches[1 + part].wait()
        for tile in range(step // LANES):
            at = pl.ds(part * step + tile * LANES, LANES)
            r = res[:, at]
            rw = r * weights[:, at]
            acc[0] += rw * r
            for d in range(1, 5):
                acc[d] += rw * pltpu.roll(r, HIST - d, 0)
    for copy in small:
        copy.wait()
    lane = iota((HIST, LANES), 1)
    sub = iota((HIST, LANES), 0)
    placed = jnp.zeros((HIST, LANES), f32)
    for d in range(HIST):
        if d < 5:
            sums = jnp.broadcast_to(jnp.sum(acc[d], axis=1, keepdims=True), (HIST, LANES))
        else:
            sums = jnp.broadcast_to(jnp.sum(acc[HIST - d], axis=1, keepdims=True), (HIST, LANES))
            sums = pltpu.roll(sums, HIST - d, 0)
        here = ((lane >> 3) == sub) & ((lane & 7) == ((sub + d) & 7))
        placed = jnp.where(here, sums, placed)
    slots = slots_of(atoms[...], table[...])
    slots = jnp.concatenate([jnp.zeros((1, BATCHES), f32), slots], axis=1)
    row = jnp.sum(placed, axis=0, keepdims=True) + slots
    out[...] = jnp.broadcast_to(row, (SIDE, LANES))
    last.wait()


def history_moments_kernel(res, weights, basis, sent, rows, out):
    lane = iota((HIST, LANES), 1)
    ends = jnp.zeros((HIST, LANES), f32)
    for i4 in range(4):
        acc = [jnp.zeros((HIST, LANES), f32) for _ in range(3)]
        for b in range(BATCHES):
            at = [pl.ds(b * WIDTH + half * LANES, LANES) for half in range(2)]
            for i in (i4, i4 + 4):
                wr = [res[i : i + 1, h] * weights[:, h] for h in at]
                place = b if i < 4 else b + BATCHES
                for t in range(3):
                    rows_t = pl.ds(TOPS[t], 8)
                    total = basis[rows_t, at[0]] * wr[0] + basis[rows_t, at[1]] * wr[1]
                    sums = jnp.sum(total, axis=1, keepdims=True)
                    acc[t] = jnp.where(lane == place, sums, acc[t])
            if i4 == 0:
                total = sum(res[:, h] * (weights[:, h] * basis[24:25, h]) for h in at)
                sums = jnp.sum(total, axis=1, keepdims=True)
                ends = jnp.where(lane == b, sums, ends)
        for peer in range(SIDE):
            for t in range(3):
                out[peer, pl.ds(24 * i4 + 8 * t, 8), :] = acc[t]
    ends = ends[0:4] + swap(ends)[4:8]
    for peer in range(SIDE):
        out[peer, pl.ds(96, 4), :] = ends
    note = jnp.sum(rows[...], axis=0, keepdims=True)
    note = first_row(jnp.where(left_half(1), note, sent[0:1, :]))
    for peer in range(SIDE):
        out[peer, pl.ds(NOTE, 4), :] = note[0:4]


def solve(matrix):
    lane = iota((HIST, LANES), 1)
    sub = iota((HIST, LANES), 0)
    eye = lane == sub
    trace = jnp.sum(jnp.where(eye, matrix, 0.0), axis=(0, 1), keepdims=True)
    ridge = ridge_share * trace / HIST
    m = jnp.where(eye, matrix + ridge, matrix)
    m = jnp.where(lane == HIST, 1.0, m)
    for j in range(HIST):
        pivot_row = m[j : j + 1, :] / m[j : j + 1, j : j + 1]
        m = jnp.where(sub == j, pivot_row, m - m[:, j : j + 1] * pivot_row)
    z = m[:, HIST : HIST + 1]
    return jnp.broadcast_to(z / jnp.sum(z, axis=0, keepdims=True), (HIST, LANES))


def split3(value):
    hi = value.astype(bf16)
    rest = value - hi.astype(f32)
    mid = rest.astype(bf16)
    lo = (rest - mid.astype(f32)).astype(bf16)
    return jnp.concatenate([hi, mid, lo], axis=0)


def add_terms(product):
    return product[0:32] + product[32:64] + product[64:96]


def first_row(value):
    return jnp.where(iota((8, LANES), 0) == 0, jnp.broadcast_to(value, (8, LANES)), 0.0)


def mixed_history(coeffs, history):
    left = left_half(1)
    c = [jnp.where(left, coeffs[i : i + 1], coeffs[i + 4 : i + 5]) for i in range(4)]
    tiles = []
    for q in range(SIDE // 2):
        halves = []
        for m in (2 * q, 2 * q + 1):
            body = sum(history[m, 24 * i : 24 * i + 24, :] * c[i] for i in range(4))
            last = sum(history[m, 96 + i : 97 + i, :] * c[i] for i in range(4))
            halves.append((body + swap(body), last + swap(last)))
        body = jnp.where(left_half(24), halves[0][0], halves[1][0])
        last = jnp.where(left, halves[0][1], halves[1][1])
        tiles.append(jnp.concatenate([body, first_row(last)], axis=0))
    return tiles


def in_pairs(rows):
    left = left_half(1)
    return [jnp.where(left, swap(rows[2 * q]), rows[2 * q + 1]) for q in range(SIDE // 2)]


def known_slots(history):
    rows = [history[m, NOTE : NOTE + 1, :] for m in range(SIDE)]
    down = jnp.transpose(jnp.concatenate(rows, axis=0))[LANES - BATCHES :, :]
    return down, in_pairs(rows)


def to_targets(sums, out):
    left = left_half(16)
    for q in range(SIDE // 2):
        low = sums[0:16, q * LANES : (q + 1) * LANES]
        high = sums[16:32, q * LANES : (q + 1) * LANES]
        out[2 * q, 0:16, :] = jnp.where(left, low, swap(high))
        out[2 * q + 1, 0:16, :] = jnp.where(left, swap(low), high)


def first_route_kernel(history, rows, out, same, matrix_out, coeffs_out):
    note = history[0, NOTE : NOTE + 1, :]
    for m in range(1, SIDE):
        note = note + history[m, NOTE : NOTE + 1, :]
    wide = jnp.broadcast_to(note, (HIST, LANES))
    sub = iota((HIST, LANES), 0)
    matrix = wide
    for i in range(1, HIST):
        matrix = jnp.where(sub == i, pltpu.roll(wide, LANES - HIST * i, 1), matrix)
    matrix = jnp.where(iota((HIST, LANES), 1) < HIST, matrix, 0.0)
    matrix_out[...] = matrix
    coeffs = solve(matrix)
    coeffs_out[...] = coeffs

    down, _ = known_slots(history)
    wanted = in_pairs([rows[m : m + 1, :] for m in range(SIDE)])
    for i in range(SIDE):
        mine = jnp.broadcast_to(down[:, i : i + 1], (BATCHES, LANES))
        for q in range(SIDE // 2):
            hit = jnp.where(mine == wanted[q], 1.0, 0.0)
            same[pl.ds(i * BATCHES, BATCHES), pl.ds(q * LANES, LANES)] = hit.astype(bf16)

    terms = split3(jnp.concatenate(mixed_history(coeffs, history), axis=1))
    to_targets(add_terms(jnp.dot(terms, same[...], preferred_element_type=f32)), out)


def row_sum_kernel(pieces, out):
    row = pieces[0, 15:16, :]
    for m in range(1, SIDE):
        row = row + pieces[m, 15:16, :]
    out[...] = jnp.broadcast_to(row, (SIDE, LANES))


def last_route_kernel(
    where, place, rows, matrix_in, history, pieces, same, out, coeffs_out, low_hot
):
    slot, first = where[0], place[0]
    row = swap(jnp.sum(rows[...], axis=0, keepdims=True))
    row = jnp.broadcast_to(row, (HIST, LANES))
    lane = iota((HIST, LANES), 1)
    sub = iota((HIST, LANES), 0)
    column = jnp.sum(jnp.where(lane == sub, row, 0.0), axis=1, keepdims=True)
    matrix = jnp.where(sub == slot, row, jnp.where(lane == slot, column, matrix_in[...]))
    matrix = jnp.where(lane < HIST, matrix, 0.0)
    coeffs = solve(matrix)
    coeffs_out[...] = coeffs
    fresh = jnp.sum(jnp.where(sub == slot, coeffs, 0.0), axis=0, keepdims=True)

    tiles = mixed_history(jnp.where(sub == slot, 0.0, coeffs), history)
    left = left_half(16)
    for q in range(SIDE // 2):
        a, b = pieces[2 * q], pieces[2 * q + 1]
        low = jnp.where(left, a, swap(b))
        high = jnp.where(left, swap(a), b)
        new = jnp.concatenate([low, high[0:8], first_row(high[8:9])], axis=0)
        tiles[q] = tiles[q] + fresh * new
    terms = split3(jnp.concatenate(tiles, axis=1))
    to_targets(add_terms(jnp.dot(terms, same[...], preferred_element_type=f32)), out)

    down, along = known_slots(history)
    low_bits = down.astype(jnp.int32) & 127
    for i in range(SIDE):
        mine = jnp.broadcast_to(low_bits[:, i : i + 1], (BATCHES, LANES))
        hit = jnp.where(mine == iota((BATCHES, LANES), 1), 1.0, 0.0)
        low_hot[pl.ds(i * BATCHES, BATCHES), :] = hit.astype(bf16)
    high_bits = jnp.concatenate(along, axis=1).astype(jnp.int32) >> 7
    masked = []
    for c in range(2):
        pick = jnp.where(high_bits == first + 4 * c, 1.0, 0.0)
        masked.append(terms * jnp.broadcast_to(pick, (96, KNOWN)).astype(bf16))
    product = jnp.dot(
        jnp.concatenate(masked, axis=0), low_hot[...], preferred_element_type=f32
    )
    left = left_half(1)
    for c in range(2):
        sums = add_terms(product[96 * c : 96 * c + 96])
        end = sums[24:25]
        for z in range(SIDE // 2):
            m = 2 * z + c
            out[m, 16:FINAL, :] = sums[0:24]
            out[m, 9:10, :] = jnp.where(left, out[m, 9:10, :], swap(end))
            out[m, 10:11, :] = jnp.where(left, out[m, 10:11, :], end)


def at_batches(received, scales):
    total = received[0, 0:16, :]
    for m in range(1, SIDE):
        total = total + received[m, 0:16, :]
    return jnp.concatenate([total, swap(total)], axis=0) * scales


def damped(scale):
    k = iota((32, LANES), 0)
    value = jnp.full((32, LANES), float(damping_table[0]), f32)
    for degree in range(1, 5):
        value = jnp.where(k >= degree * degree, float(np.float32(1.0 / (1 + degree))), value)
    return jnp.where(k < COMPS, value * scale, 0.0)


def correction(at, b):
    return [
        jnp.broadcast_to(at[TOPS[t] : TOPS[t] + HEIGHTS[t], b : b + 1], (HEIGHTS[t], LANES))
        for t in range(4)
    ]


def correct_tile(wide, basis):
    terms = sum(wide[t] * basis[t] for t in range(3))
    return jnp.sum(terms, axis=0, keepdims=True) + wide[3] * basis[3]


def basis_tiles(basis, here):
    return [basis[pl.ds(TOPS[t], HEIGHTS[t]), here] for t in range(4)]


def update_kernel(
    scale, where, received, coeffs_in, basis, res, rho, weights, target, coupling,
    out, mixed_out, weighted,
):
    at = at_batches(received, damped(scale))
    coeffs = coeffs_in[...]
    slot = where[0]
    sub = iota((HIST, LANES), 0)
    lane = iota((HIST, LANES), 1)
    overlap = jnp.zeros((HIST, LANES), f32)
    for b in range(BATCHES):
        wide = correction(at, b)
        for half in range(2):
            here = pl.ds(b * WIDTH + half * LANES, LANES)
            r = res[:, here]
            mixed = rho[:, here] + mixing_beta * r
            density = jnp.sum(coeffs * mixed, axis=0, keepdims=True)
            density = density - mixing_beta * correct_tile(wide, basis_tiles(basis, here))
            res_new = target[:, here] + coupling[:, here] * jnp.tanh(density) - density
            mixed_out[:, here] = jnp.where(sub == slot, density + mixing_beta * res_new, mixed)
            wr = weights[:, here] * res_new
            weighted[:, here] = wr
            overlap = overlap + jnp.where(sub == slot, res_new, r) * wr
    acc = [jnp.zeros((h, LANES), f32) for h in HEIGHTS]
    for b in range(BATCHES):
        total = [None] * 4
        for half in range(2):
            here = pl.ds(b * WIDTH + half * LANES, LANES)
            wr = weighted[:, here]
            y = basis_tiles(basis, here)
            for t in range(4):
                total[t] = y[t] * wr if half == 0 else total[t] + y[t] * wr
        for t in range(4):
            sums = jnp.sum(total[t], axis=1, keepdims=True)
            place = b if t < 2 else b + BATCHES
            acc[t] = jnp.where(lane[: HEIGHTS[t]] == place, sums, acc[t])
    sums = jnp.sum(overlap, axis=1, keepdims=True)
    row = jnp.sum(jnp.where(lane == sub + BATCHES, sums, 0.0), axis=0, keepdims=True)
    row = jnp.broadcast_to(row, (8, LANES))
    end = jnp.where(sub == 7, row, first_row(acc[3]))
    packed = jnp.concatenate([acc[0] + acc[2], acc[1] + end], axis=0)
    for peer in range(SIDE):
        out[peer] = packed


def quarter_kernel(scale, received, out):
    total = received[0]
    for m in range(1, SIDE):
        total = total + received[m]
    total = total * scale
    end = jnp.where(left_half(1), swap(total[9:10]), total[10:11])
    for y in range(4):
        out[y, 0:24, :] = total[16:FINAL]
        out[y, 24:32, :] = first_row(end)


def final_kernel(scale, received, coeffs_in, basis, mixed, quarters, density_out, moments_out):
    at = at_batches(received, damped(scale))
    coeffs = coeffs_in[...]
    for b in range(BATCHES):
        wide = correction(at, b)
        for half in range(2):
            here = pl.ds(b * WIDTH + half * LANES, LANES)
            density = jnp.sum(coeffs * mixed[:, here], axis=0, keepdims=True)
            correct = correct_tile(wide, basis_tiles(basis, here))
            density_out[:, here] = density - mixing_beta * correct
    for y in range(4):
        moments_out[:, pl.ds(y * QUARTER, QUARTER)] = quarters[y, 0:COMPS, :]


def exchange(pieces, axes):
    return lax.all_to_all(pieces, axes, 0, 0, tiled=True)


def local(
    weights,
    target,
    coupling,
    multipole_basis,
    rho_hist,
    res_hist,
    batch_atom,
    owner_slot,
    slot_index,
):
    points = weights.shape[0]
    owned_count = owner_slot.shape[0] // lax.axis_size(ATOM)
    atom_points = points * lax.axis_size(GRID) // owned_count
    scale = 1.0 / math.sqrt(atom_points)
    assert points == POINTS and owned_count == OWNED and multipole_basis.shape[0] == COMPS

    weights, target, coupling = (v.reshape(1, points) for v in (weights, target, coupling))
    atoms = batch_atom.reshape(1, BATCHES)
    table = owner_slot.reshape(-1, LANES)
    place = (lax.axis_index("x") * 8 + lax.axis_index("y")).astype(jnp.int32).reshape(1)
    atoms, place, where = lax.optimization_barrier((atoms, place, slot_index[0:1]))

    sent, res_hist, weights, multipole_basis = call(
        gram_kernel,
        (shape(SIDE, LANES), shape(HIST, POINTS), shape(1, POINTS), shape(COMPS, POINTS)),
        [pltpu.HBM] * 5,
        scratch=[
            pltpu.VMEM((1, BATCHES), jnp.int32),
            pltpu.VMEM((32, LANES), jnp.int32),
            pltpu.SemaphoreType.DMA((4 + PARTS,)),
        ],
    )(*(
        pltpu.with_memory_space_constraint(v, pltpu.HBM)
        for v in (res_hist, weights, atoms, table, multipole_basis)
    ))
    rows = exchange(sent, COL)
    history = call(history_moments_kernel, shape(SIDE, PACKED, LANES), [V] * 5)(
        res_hist, weights, multipole_basis, sent, rows
    )
    history = exchange(history, ROW)
    pieces, same, matrix, coeffs = call(
        first_route_kernel,
        (
            shape(SIDE, 16, LANES),
            shape(KNOWN, KNOWN, dtype=bf16),
            shape(HIST, LANES),
            shape(HIST, LANES),
        ),
        [V] * 2,
    )(history, rows)
    received = exchange(pieces, COL)

    pieces, mixed = call(
        functools.partial(update_kernel, scale),
        (shape(SIDE, 16, LANES), shape(HIST, POINTS)),
        [S] + [V] * 8,
        scratch=[pltpu.VMEM((1, POINTS), f32)],
    )(where, received, coeffs, multipole_basis, res_hist, rho_hist, weights, target, coupling)
    pieces = exchange(pieces, ROW)
    rows = call(row_sum_kernel, shape(SIDE, LANES), [V])(pieces)
    rows = exchange(rows, COL)
    routed, coeffs = call(
        last_route_kernel,
        (shape(SIDE, FINAL, LANES), shape(HIST, LANES)),
        [S, S] + [V] * 5,
        scratch=[pltpu.VMEM((KNOWN, LANES), bf16)],
    )(where, place, rows, matrix, history, pieces, same)
    received = exchange(routed, COL)
    quarters = call(functools.partial(quarter_kernel, scale), shape(4, 32, LANES), [V])(received)
    quarters = exchange(quarters, ("y",))
    density, moments = call(
        functools.partial(final_kernel, scale), (shape(1, POINTS), shape(COMPS, OWNED)), [V] * 5
    )(received, coeffs, multipole_basis, mixed, quarters)
    return density.reshape(points), moments


def solution(mesh):
    torus = Mesh(mesh.devices.reshape(8, 4, 4, 2), AXES)
    placed = (
        P(AXES),
        P(AXES),
        P(AXES),
        P(None, AXES),
        P(None, AXES),
        P(None, AXES),
        P(AXES),
        P(),
        P(),
    )
    return jax.shard_map(
        local, mesh=torus, in_specs=placed, out_specs=(P(AXES), P(None, ATOM)), check_vma=False
    )
```

```python
import functools
import math

import jax
import jax.numpy as jnp
import numpy as np
from jax import lax
from jax.experimental import pallas as pl
from jax.experimental.pallas import tpu as pltpu
from jax.sharding import Mesh
from jax.sharding import PartitionSpec as P

ITERS = 2
AXES = ("z", "y", "x", "c")
GRID = ("z", "y")
ATOM = ("x", "c")
COL = ("z", "c")
ROW = ("y", "x")

damping_table = np.array(
    [1.0 / (1 + degree) for degree in range(5) for order in range(2 * degree + 1)], dtype=np.float32
)
mixing_beta = 0.5
ridge_share = 0.1

LANES = 128
HIST = 8
COMPS = 25
BATCHES = 64
WIDTH = 256
POINTS = BATCHES * WIDTH
SIDE = 16
KNOWN = SIDE * BATCHES
OWNED = 512
PACKED = 104
NOTE = 100
FINAL = 40
QUARTER = OWNED // 4
PARTS = 4

f32 = jnp.float32
bf16 = jnp.bfloat16


def iota(shape, dim):
    return lax.broadcasted_iota(jnp.int32, shape, dim)


def call(kernel, out_shape, in_specs, *, scratch=(), vmem=12 << 20, cost=20000):
    return pl.pallas_call(
        kernel,
        out_shape=out_shape,
        in_specs=[pl.BlockSpec(memory_space=s) for s in in_specs],
        out_specs=jax.tree.map(lambda _: pl.BlockSpec(memory_space=pltpu.VMEM), out_shape),
        scratch_shapes=list(scratch),
        compiler_params=pltpu.CompilerParams(vmem_limit_bytes=vmem),
        cost_estimate=pl.CostEstimate(flops=cost * 1000, bytes_accessed=1 << 20, transcendentals=0),
    )


V = pltpu.VMEM
S = pltpu.SMEM


def shape(*dims, dtype=f32):
    return jax.ShapeDtypeStruct(dims, dtype)


TOPS = (0, 8, 16, 24)
HEIGHTS = (8, 8, 8, 1)


def left_half(rows):
    return iota((rows, LANES), 1) < BATCHES


def swap(value):
    return pltpu.roll(value, BATCHES, 1)


def slots_of(atoms, table):
    hits = jnp.where(iota((32, BATCHES), 0) == (atoms >> 7), 1.0, 0.0).astype(bf16)
    halves = []
    for half in (table >> 6, table & 63):
        rows = lax.dot_general(
            half.astype(f32).astype(bf16), hits, (((0,), (0,)), ((), ())),
            preferred_element_type=f32,
        )
        mine = iota((LANES, BATCHES), 0) == (atoms & 127)
        halves.append(jnp.sum(jnp.where(mine, rows, 0.0), axis=0, keepdims=True))
    return halves[0] * 64.0 + halves[1]


def gram_kernel(
    res_in, weights_in, atoms_in, table_in,
    out, res, weights,
    atoms, table, sems,
):
    def fetch(source, target, sem):
        copy = pltpu.make_async_copy(source, target, sems.at[sem])
        copy.start()
        return copy

    step = POINTS // PARTS
    fetches = [fetch(weights_in, weights, 0)]
    for part in range(PARTS):
        at = (slice(None), pl.ds(part * step, step))
        fetches.append(fetch(res_in.at[at], res.at[at], 1 + part))
    small = [fetch(atoms_in, atoms, 1 + PARTS), fetch(table_in, table, 2 + PARTS)]

    acc = [jnp.zeros((HIST, LANES), f32) for _ in range(5)]
    fetches[0].wait()
    for part in range(PARTS):
        fetches[1 + part].wait()
        for tile in range(step // LANES):
            at = pl.ds(part * step + tile * LANES, LANES)
            r = res[:, at]
            rw = r * weights[:, at]
            acc[0] += rw * r
            for d in range(1, 5):
                acc[d] += rw * pltpu.roll(r, HIST - d, 0)
    for copy in small:
        copy.wait()
    lane = iota((HIST, LANES), 1)
    sub = iota((HIST, LANES), 0)
    placed = jnp.zeros((HIST, LANES), f32)
    for d in range(HIST):
        if d < 5:
            sums = jnp.broadcast_to(jnp.sum(acc[d], axis=1, keepdims=True), (HIST, LANES))
        else:
            sums = jnp.broadcast_to(jnp.sum(acc[HIST - d], axis=1, keepdims=True), (HIST, LANES))
            sums = pltpu.roll(sums, HIST - d, 0)
        here = ((lane >> 3) == sub) & ((lane & 7) == ((sub + d) & 7))
        placed = jnp.where(here, sums, placed)
    slots = slots_of(atoms[...], table[...])
    slots = jnp.concatenate([jnp.zeros((1, BATCHES), f32), slots], axis=1)
    row = jnp.sum(placed, axis=0, keepdims=True) + slots
    out[...] = jnp.broadcast_to(row, (SIDE, LANES))


def history_moments_kernel(res, weights, basis, sent, rows, out):
    lane = iota((HIST, LANES), 1)
    ends = jnp.zeros((HIST, LANES), f32)
    for i4 in range(4):
        acc = [jnp.zeros((HIST, LANES), f32) for _ in range(3)]
        for b in range(BATCHES):
            at = [pl.ds(b * WIDTH + half * LANES, LANES) for half in range(2)]
            for i in (i4, i4 + 4):
                wr = [res[i : i + 1, h] * weights[:, h] for h in at]
                place = b if i < 4 else b + BATCHES
                for t in range(3):
                    rows_t = pl.ds(TOPS[t], 8)
                    total = basis[rows_t, at[0]] * wr[0] + basis[rows_t, at[1]] * wr[1]
                    sums = jnp.sum(total, axis=1, keepdims=True)
                    acc[t] = jnp.where(lane == place, sums, acc[t])
            if i4 == 0:
                total = sum(res[:, h] * (weights[:, h] * basis[24:25, h]) for h in at)
                sums = jnp.sum(total, axis=1, keepdims=True)
                ends = jnp.where(lane == b, sums, ends)
        for peer in range(SIDE):
            for t in range(3):
                out[peer, pl.ds(24 * i4 + 8 * t, 8), :] = acc[t]
    ends = ends[0:4] + swap(ends)[4:8]
    for peer in range(SIDE):
        out[peer, pl.ds(96, 4), :] = ends
    note = jnp.sum(rows[...], axis=0, keepdims=True)
    note = first_row(jnp.where(left_half(1), note, sent[0:1, :]))
    for peer in range(SIDE):
        out[peer, pl.ds(NOTE, 4), :] = note[0:4]


def spread(row, lane):
    return jnp.broadcast_to(row[:, lane : lane + 1], (HIST, LANES))


def solve(matrix):
    trace = matrix[0][0]
    for i in range(1, HIST):
        trace = trace + matrix[i][i]
    ridge = ridge_share * trace / HIST
    m = [[matrix[i][j] + ridge if i == j else matrix[i][j] for j in range(i + 1)] for i in range(HIST)]
    right = [jnp.ones((HIST, LANES), f32)] * HIST
    inverse = []
    for j in range(HIST):
        inverse.append(1.0 / m[j][j])
        for i in range(j + 1, HIST):
            factor = m[i][j] * inverse[j]
            right[i] = right[i] - factor * right[j]
            for k in range(j + 1, i + 1):
                m[i][k] = m[i][k] - factor * m[k][j]
    z = [None] * HIST
    for j in reversed(range(HIST)):
        value = right[j]
        for i in range(j + 1, HIST):
            value = value - m[i][j] * z[i]
        z[j] = value * inverse[j]
    total = z[0]
    for j in range(1, HIST):
        total = total + z[j]
    return [value / total for value in z]


def in_rows(coeffs):
    sub = iota((HIST, LANES), 0)
    rows = coeffs[0]
    for i in range(1, HIST):
        rows = jnp.where(sub == i, coeffs[i], rows)
    return rows


def split3(value):
    hi = value.astype(bf16)
    rest = value - hi.astype(f32)
    mid = rest.astype(bf16)
    lo = (rest - mid.astype(f32)).astype(bf16)
    return jnp.concatenate([hi, mid, lo], axis=0)


def add_terms(product):
    return product[0:32] + product[32:64] + product[64:96]


def first_row(value):
    return jnp.where(iota((8, LANES), 0) == 0, jnp.broadcast_to(value, (8, LANES)), 0.0)


def mixed_history(coeffs, history):
    left = left_half(1)
    c = [jnp.where(left_half(8), coeffs[i], coeffs[i + 4]) for i in range(4)]
    c24 = [jnp.concatenate([value] * 3, axis=0) for value in c]
    tiles = []
    for q in range(SIDE // 2):
        halves = []
        for m in (2 * q, 2 * q + 1):
            body = sum(history[m, 24 * i : 24 * i + 24, :] * c24[i] for i in range(4))
            last = sum(history[m, 96 + i : 97 + i, :] * c[i][0:1] for i in range(4))
            halves.append((body + swap(body), last + swap(last)))
        body = jnp.where(left_half(24), halves[0][0], halves[1][0])
        last = jnp.where(left, halves[0][1], halves[1][1])
        tiles.append(jnp.concatenate([body, first_row(last)], axis=0))
    return tiles


def in_pairs(rows):
    left = left_half(1)
    return [jnp.where(left, swap(rows[2 * q]), rows[2 * q + 1]) for q in range(SIDE // 2)]


def known_slots(history):
    rows = [history[m, NOTE : NOTE + 1, :] for m in range(SIDE)]
    down = jnp.transpose(jnp.concatenate(rows, axis=0))[LANES - BATCHES :, :]
    return down, in_pairs(rows)


def to_targets(sums, out):
    left = left_half(16)
    for q in range(SIDE // 2):
        low = sums[0:16, q * LANES : (q + 1) * LANES]
        high = sums[16:32, q * LANES : (q + 1) * LANES]
        out[2 * q, 0:16, :] = jnp.where(left, low, swap(high))
        out[2 * q + 1, 0:16, :] = jnp.where(left, swap(low), high)


def first_route_kernel(history, rows, out, same, matrix_out, coeffs_out):
    note = history[0, NOTE : NOTE + 1, :]
    for m in range(1, SIDE):
        note = note + history[m, NOTE : NOTE + 1, :]
    matrix_out[...] = note
    coeffs = solve([[spread(note, HIST * i + j) for j in range(i + 1)] for i in range(HIST)])
    coeffs_out[...] = in_rows(coeffs)

    down, _ = known_slots(history)
    wanted = in_pairs([rows[m : m + 1, :] for m in range(SIDE)])
    for i in range(SIDE):
        mine = jnp.broadcast_to(down[:, i : i + 1], (BATCHES, LANES))
        for q in range(SIDE // 2):
            hit = jnp.where(mine == wanted[q], 1.0, 0.0)
            same[pl.ds(i * BATCHES, BATCHES), pl.ds(q * LANES, LANES)] = hit.astype(bf16)

    terms = split3(jnp.concatenate(mixed_history(coeffs, history), axis=1))
    to_targets(add_terms(jnp.dot(terms, same[...], preferred_element_type=f32)), out)


def row_sum_kernel(pieces, out):
    row = pieces[0, 15:16, :]
    for m in range(1, SIDE):
        row = row + pieces[m, 15:16, :]
    out[...] = jnp.broadcast_to(row, (SIDE, LANES))


def last_route_kernel(
    where, place, rows, matrix_in, history, pieces, same, out, coeffs_out, low_hot
):
    slot, first = where[0], place[0]
    row = jnp.sum(rows[...], axis=0, keepdims=True)
    sub = iota((HIST, LANES), 0)
    old = matrix_in[...]
    new = [spread(row, BATCHES + i) for i in range(HIST)]
    coeffs = solve(
        [
            [
                jnp.where(slot == i, new[j], jnp.where(slot == j, new[i], spread(old, HIST * i + j)))
                for j in range(i + 1)
            ]
            for i in range(HIST)
        ]
    )
    coeffs_out[...] = in_rows(coeffs)
    fresh = jnp.where(slot == 0, coeffs[0], 0.0)
    for i in range(1, HIST):
        fresh = jnp.where(slot == i, coeffs[i], fresh)
    kept = [jnp.where(slot == i, 0.0, coeffs[i]) for i in range(HIST)]
    fresh = jnp.concatenate([fresh] * 4, axis=0)

    tiles = mixed_history(kept, history)
    left = left_half(16)
    for q in range(SIDE // 2):
        a, b = pieces[2 * q], pieces[2 * q + 1]
        low = jnp.where(left, a, swap(b))
        high = jnp.where(left, swap(a), b)
        new = jnp.concatenate([low, high[0:8], first_row(high[8:9])], axis=0)
        tiles[q] = tiles[q] + fresh * new
    terms = split3(jnp.concatenate(tiles, axis=1))
    to_targets(add_terms(jnp.dot(terms, same[...], preferred_element_type=f32)), out)

    down, along = known_slots(history)
    low_bits = down.astype(jnp.int32) & 127
    for i in range(SIDE):
        mine = jnp.broadcast_to(low_bits[:, i : i + 1], (BATCHES, LANES))
        hit = jnp.where(mine == iota((BATCHES, LANES), 1), 1.0, 0.0)
        low_hot[pl.ds(i * BATCHES, BATCHES), :] = hit.astype(bf16)
    high_bits = jnp.concatenate(along, axis=1).astype(jnp.int32) >> 7
    masked = []
    for c in range(2):
        pick = jnp.where(high_bits == first + 4 * c, 1.0, 0.0)
        masked.append(terms * jnp.broadcast_to(pick, (96, KNOWN)).astype(bf16))
    product = jnp.dot(
        jnp.concatenate(masked, axis=0), low_hot[...], preferred_element_type=f32
    )
    left = left_half(1)
    for c in range(2):
        sums = add_terms(product[96 * c : 96 * c + 96])
        end = sums[24:25]
        for z in range(SIDE // 2):
            m = 2 * z + c
            out[m, 16:FINAL, :] = sums[0:24]
            out[m, 9:10, :] = jnp.where(left, out[m, 9:10, :], swap(end))
            out[m, 10:11, :] = jnp.where(left, out[m, 10:11, :], end)


def at_batches(received, scales):
    total = received[0, 0:16, :]
    for m in range(1, SIDE):
        total = total + received[m, 0:16, :]
    return jnp.concatenate([total, swap(total)], axis=0) * scales


def damped(scale):
    k = iota((32, LANES), 0)
    value = jnp.full((32, LANES), float(damping_table[0]), f32)
    for degree in range(1, 5):
        value = jnp.where(k >= degree * degree, float(np.float32(1.0 / (1 + degree))), value)
    return jnp.where(k < COMPS, value * scale, 0.0)


def correction(at, b):
    return [
        jnp.broadcast_to(at[TOPS[t] : TOPS[t] + HEIGHTS[t], b : b + 1], (HEIGHTS[t], LANES))
        for t in range(4)
    ]


def correct_tile(wide, basis):
    terms = sum(wide[t] * basis[t] for t in range(3))
    return jnp.sum(terms, axis=0, keepdims=True) + wide[3] * basis[3]


def basis_tiles(basis, here):
    return [basis[pl.ds(TOPS[t], HEIGHTS[t]), here] for t in range(4)]


def update_kernel(
    scale, where, received, coeffs_in, basis, res, rho, weights, target, coupling,
    out, mixed_out, weighted,
):
    at = at_batches(received, damped(scale))
    coeffs = coeffs_in[...]
    slot = where[0]
    sub = iota((HIST, LANES), 0)
    lane = iota((HIST, LANES), 1)
    overlap = jnp.zeros((HIST, LANES), f32)
    for b in range(BATCHES):
        wide = correction(at, b)
        for half in range(2):
            here = pl.ds(b * WIDTH + half * LANES, LANES)
            r = res[:, here]
            mixed = rho[:, here] + mixing_beta * r
            density = jnp.sum(coeffs * mixed, axis=0, keepdims=True)
            density = density - mixing_beta * correct_tile(wide, basis_tiles(basis, here))
            res_new = target[:, here] + coupling[:, here] * jnp.tanh(density) - density
            mixed_out[:, here] = jnp.where(sub == slot, density + mixing_beta * res_new, mixed)
            wr = weights[:, here] * res_new
            weighted[:, here] = wr
            overlap = overlap + jnp.where(sub == slot, res_new, r) * wr
    acc = [jnp.zeros((h, LANES), f32) for h in HEIGHTS]
    for b in range(BATCHES):
        total = [None] * 4
        for half in range(2):
            here = pl.ds(b * WIDTH + half * LANES, LANES)
            wr = weighted[:, here]
            y = basis_tiles(basis, here)
            for t in range(4):
                total[t] = y[t] * wr if half == 0 else total[t] + y[t] * wr
        for t in range(4):
            sums = jnp.sum(total[t], axis=1, keepdims=True)
            place = b if t < 2 else b + BATCHES
            acc[t] = jnp.where(lane[: HEIGHTS[t]] == place, sums, acc[t])
    sums = jnp.sum(overlap, axis=1, keepdims=True)
    row = jnp.sum(jnp.where(lane == sub + BATCHES, sums, 0.0), axis=0, keepdims=True)
    row = jnp.broadcast_to(row, (8, LANES))
    end = jnp.where(sub == 7, row, first_row(acc[3]))
    packed = jnp.concatenate([acc[0] + acc[2], acc[1] + end], axis=0)
    for peer in range(SIDE):
        out[peer] = packed


def quarter_kernel(scale, received, out):
    total = received[0]
    for m in range(1, SIDE):
        total = total + received[m]
    total = total * scale
    end = jnp.where(left_half(1), swap(total[9:10]), total[10:11])
    out[0:24, :] = total[16:FINAL]
    out[24:32, :] = first_row(end)


def density_kernel(scale, received, coeffs_in, basis, mixed, density_out):
    at = at_batches(received, damped(scale))
    coeffs = coeffs_in[...]
    for b in range(BATCHES):
        wide = correction(at, b)
        for half in range(2):
            here = pl.ds(b * WIDTH + half * LANES, LANES)
            density = jnp.sum(coeffs * mixed[:, here], axis=0, keepdims=True)
            correct = correct_tile(wide, basis_tiles(basis, here))
            density_out[:, here] = density - mixing_beta * correct


def owned_kernel(place, mine, one, two, three, moments_out):
    y = place[1]
    for step, quarter in enumerate((mine, one, two, three)):
        at = pl.multiple_of(((y + 4 - step) & 3) * QUARTER, QUARTER)
        moments_out[:, pl.ds(at, QUARTER)] = quarter[0:COMPS, :]


def exchange(pieces, axes):
    return lax.all_to_all(pieces, axes, 0, 0, tiled=True)


def local(
    weights,
    target,
    coupling,
    multipole_basis,
    rho_hist,
    res_hist,
    batch_atom,
    owner_slot,
    slot_index,
):
    points = weights.shape[0]
    owned_count = owner_slot.shape[0] // lax.axis_size(ATOM)
    atom_points = points * lax.axis_size(GRID) // owned_count
    scale = 1.0 / math.sqrt(atom_points)
    assert points == POINTS and owned_count == OWNED and multipole_basis.shape[0] == COMPS

    weights, target, coupling = (v.reshape(1, points) for v in (weights, target, coupling))
    atoms = batch_atom.reshape(1, BATCHES)
    table = owner_slot.reshape(-1, LANES)
    y = lax.axis_index("y").astype(jnp.int32)
    place = jnp.stack([lax.axis_index("x").astype(jnp.int32) * 8 + y, y])
    atoms, place, where = lax.optimization_barrier((atoms, place, slot_index[0:1]))

    sent, res_hist, weights = call(
        gram_kernel,
        (shape(SIDE, LANES), shape(HIST, POINTS), shape(1, POINTS)),
        [pltpu.HBM] * 4,
        scratch=[
            pltpu.VMEM((1, BATCHES), jnp.int32),
            pltpu.VMEM((32, LANES), jnp.int32),
            pltpu.SemaphoreType.DMA((4 + PARTS,)),
        ],
        cost=6000000,
    )(*(
        pltpu.with_memory_space_constraint(v, pltpu.HBM)
        for v in (res_hist, weights, atoms, table)
    ))
    rows = exchange(sent, COL)
    history = call(history_moments_kernel, shape(SIDE, PACKED, LANES), [V] * 5)(
        res_hist, weights, multipole_basis, sent, rows
    )
    history = exchange(history, ROW)
    pieces, same, matrix, coeffs = call(
        first_route_kernel,
        (
            shape(SIDE, 16, LANES),
            shape(KNOWN, KNOWN, dtype=bf16),
            shape(1, LANES),
            shape(HIST, LANES),
        ),
        [V] * 2,
    )(history, rows)
    received = exchange(pieces, COL)

    pieces, mixed = call(
        functools.partial(update_kernel, scale),
        (shape(SIDE, 16, LANES), shape(HIST, POINTS)),
        [S] + [V] * 8,
        scratch=[pltpu.VMEM((1, POINTS), f32)],
    )(where, received, coeffs, multipole_basis, res_hist, rho_hist, weights, target, coupling)
    pieces = exchange(pieces, ROW)
    rows = call(row_sum_kernel, shape(SIDE, LANES), [V])(pieces)
    rows = exchange(rows, COL)
    routed, coeffs = call(
        last_route_kernel,
        (shape(SIDE, FINAL, LANES), shape(HIST, LANES)),
        [S, S] + [V] * 5,
        scratch=[pltpu.VMEM((KNOWN, LANES), bf16)],
    )(where, place, rows, matrix, history, pieces, same)
    received = exchange(routed, COL)
    mine = call(functools.partial(quarter_kernel, scale), shape(32, LANES), [V])(received)
    others = [
        lax.ppermute(mine, "y", [(i, (i + step) % 4) for i in range(4)]) for step in (1, 2, 3)
    ]
    density = call(functools.partial(density_kernel, scale), shape(1, POINTS), [V] * 4)(
        received, coeffs, multipole_basis, mixed
    )
    moments = call(owned_kernel, shape(COMPS, OWNED), [S] + [V] * 4)(place, mine, *others)
    return density.reshape(points), moments


def solution(mesh):
    torus = Mesh(mesh.devices.reshape(8, 4, 4, 2), AXES)
    placed = (
        P(AXES),
        P(AXES),
        P(AXES),
        P(None, AXES),
        P(None, AXES),
        P(None, AXES),
        P(AXES),
        P(),
        P(),
    )
    return jax.shard_map(
        local, mesh=torus, in_specs=placed, out_specs=(P(AXES), P(None, ATOM)), check_vma=False
    )
```

```python
import functools
import math

import jax
import jax.numpy as jnp
import numpy as np
from jax import lax
from jax.experimental import pallas as pl
from jax.experimental.pallas import tpu as pltpu
from jax.sharding import Mesh
from jax.sharding import PartitionSpec as P

ITERS = 2
AXES = ("z", "y", "x", "c")
GRID = ("z", "y")
ATOM = ("x", "c")
COL = ("z", "c")
ROW = ("y", "x")

damping_table = np.array(
    [1.0 / (1 + degree) for degree in range(5) for order in range(2 * degree + 1)], dtype=np.float32
)
mixing_beta = 0.5
ridge_share = 0.1

LANES = 128
HIST = 8
COMPS = 25
BATCHES = 64
WIDTH = 256
POINTS = BATCHES * WIDTH
SIDE = 16
KNOWN = SIDE * BATCHES
OWNED = 512
PIECE = 13
NOTE = 100
PACKED = 101
FINAL = 38
QUARTER = OWNED // 4
PARTS = 4

f32 = jnp.float32
bf16 = jnp.bfloat16


def iota(shape, dim):
    return lax.broadcasted_iota(jnp.int32, shape, dim)


def call(kernel, out_shape, in_specs, *, scratch=(), vmem=12 << 20, cost=20000):
    return pl.pallas_call(
        kernel,
        out_shape=out_shape,
        in_specs=[pl.BlockSpec(memory_space=s) for s in in_specs],
        out_specs=jax.tree.map(lambda _: pl.BlockSpec(memory_space=pltpu.VMEM), out_shape),
        scratch_shapes=list(scratch),
        compiler_params=pltpu.CompilerParams(vmem_limit_bytes=vmem),
        cost_estimate=pl.CostEstimate(flops=cost * 1000, bytes_accessed=1 << 20, transcendentals=0),
    )


V = pltpu.VMEM
S = pltpu.SMEM


def shape(*dims, dtype=f32):
    return jax.ShapeDtypeStruct(dims, dtype)


TOPS = (0, 8, 16, 24)
HEIGHTS = (8, 8, 8, 1)


def left_half(rows):
    return iota((rows, LANES), 1) < BATCHES


def swap(value):
    return pltpu.roll(value, BATCHES, 1)


def slots_of(atoms, table):
    hits = jnp.where(iota((32, BATCHES), 0) == (atoms >> 7), 1.0, 0.0).astype(bf16)
    halves = []
    for half in (table >> 6, table & 63):
        rows = lax.dot_general(
            half.astype(f32).astype(bf16), hits, (((0,), (0,)), ((), ())),
            preferred_element_type=f32,
        )
        mine = iota((LANES, BATCHES), 0) == (atoms & 127)
        halves.append(jnp.sum(jnp.where(mine, rows, 0.0), axis=0, keepdims=True))
    return halves[0] * 64.0 + halves[1]


def gram_kernel(
    res_in, weights_in, atoms_in, table_in,
    out, res, weights,
    atoms, table, sems,
):
    def fetch(source, target, sem):
        copy = pltpu.make_async_copy(source, target, sems.at[sem])
        copy.start()
        return copy

    step = POINTS // PARTS
    fetches = [fetch(weights_in, weights, 0)]
    for part in range(PARTS):
        at = (slice(None), pl.ds(part * step, step))
        fetches.append(fetch(res_in.at[at], res.at[at], 1 + part))
    small = [fetch(atoms_in, atoms, 1 + PARTS), fetch(table_in, table, 2 + PARTS)]

    acc = [jnp.zeros((HIST, LANES), f32) for _ in range(5)]
    fetches[0].wait()
    for part in range(PARTS):
        fetches[1 + part].wait()
        for tile in range(step // LANES):
            at = pl.ds(part * step + tile * LANES, LANES)
            r = res[:, at]
            rw = r * weights[:, at]
            acc[0] += rw * r
            for d in range(1, 5):
                acc[d] += rw * pltpu.roll(r, HIST - d, 0)
    for copy in small:
        copy.wait()
    lane = iota((HIST, LANES), 1)
    sub = iota((HIST, LANES), 0)
    placed = jnp.zeros((HIST, LANES), f32)
    for d in range(HIST):
        if d < 5:
            sums = jnp.broadcast_to(jnp.sum(acc[d], axis=1, keepdims=True), (HIST, LANES))
        else:
            sums = jnp.broadcast_to(jnp.sum(acc[HIST - d], axis=1, keepdims=True), (HIST, LANES))
            sums = pltpu.roll(sums, HIST - d, 0)
        here = ((lane >> 3) == sub) & ((lane & 7) == ((sub + d) & 7))
        placed = jnp.where(here, sums, placed)
    slots = slots_of(atoms[...], table[...])
    slots = jnp.concatenate([jnp.zeros((1, BATCHES), f32), slots], axis=1)
    out[...] = jnp.sum(placed, axis=0, keepdims=True) + slots


def repeat_kernel(row, out):
    out[...] = jnp.broadcast_to(row[...], (SIDE, LANES))


def history_moments_kernel(res, weights, basis, sent, rows, out, whole):
    lane = iota((HIST, LANES), 1)
    ends = jnp.zeros((HIST, LANES), f32)
    for i4 in range(4):
        acc = [jnp.zeros((HIST, LANES), f32) for _ in range(3)]
        for b in range(BATCHES):
            at = [pl.ds(b * WIDTH + half * LANES, LANES) for half in range(2)]
            for i in (i4, i4 + 4):
                wr = [res[i : i + 1, h] * weights[:, h] for h in at]
                place = b if i < 4 else b + BATCHES
                for t in range(3):
                    rows_t = pl.ds(TOPS[t], 8)
                    total = basis[rows_t, at[0]] * wr[0] + basis[rows_t, at[1]] * wr[1]
                    sums = jnp.sum(total, axis=1, keepdims=True)
                    acc[t] = jnp.where(lane == place, sums, acc[t])
            if i4 == 0:
                total = sum(res[:, h] * (weights[:, h] * basis[24:25, h]) for h in at)
                sums = jnp.sum(total, axis=1, keepdims=True)
                ends = jnp.where(lane == b, sums, ends)
        for t in range(3):
            whole[pl.ds(24 * i4 + 8 * t, 8), :] = acc[t]
    whole[pl.ds(96, 8), :] = jnp.where(
        iota((8, LANES), 0) < 4, ends + pltpu.roll(swap(ends), 4, 0), 0.0
    )
    note = jnp.sum(rows[...], axis=0, keepdims=True)
    whole[NOTE : NOTE + 1, :] = jnp.where(left_half(1), note, sent[...])
    for peer in range(SIDE):
        out[PACKED * peer : PACKED * (peer + 1), :] = whole[0:PACKED, :]


def spread(row, lane):
    return jnp.broadcast_to(row[:, lane : lane + 1], (HIST, LANES))


def solve(matrix):
    trace = matrix[0][0]
    for i in range(1, HIST):
        trace = trace + matrix[i][i]
    ridge = ridge_share * trace / HIST
    m = [[matrix[i][j] + ridge if i == j else matrix[i][j] for j in range(i + 1)] for i in range(HIST)]
    right = [jnp.ones((HIST, LANES), f32)] * HIST
    inverse = []
    for j in range(HIST):
        inverse.append(1.0 / m[j][j])
        for i in range(j + 1, HIST):
            factor = m[i][j] * inverse[j]
            right[i] = right[i] - factor * right[j]
            for k in range(j + 1, i + 1):
                m[i][k] = m[i][k] - factor * m[k][j]
    z = [None] * HIST
    for j in reversed(range(HIST)):
        value = right[j]
        for i in range(j + 1, HIST):
            value = value - m[i][j] * z[i]
        z[j] = value * inverse[j]
    total = z[0]
    for j in range(1, HIST):
        total = total + z[j]
    return [value / total for value in z]


def in_rows(coeffs):
    sub = iota((HIST, LANES), 0)
    rows = coeffs[0]
    for i in range(1, HIST):
        rows = jnp.where(sub == i, coeffs[i], rows)
    return rows


def split3(value):
    hi = value.astype(bf16)
    rest = value - hi.astype(f32)
    mid = rest.astype(bf16)
    lo = (rest - mid.astype(f32)).astype(bf16)
    return jnp.concatenate([hi, mid, lo], axis=0)


def add_terms(product):
    return product[0:32] + product[32:64] + product[64:96]


def first_row(value):
    return jnp.where(iota((8, LANES), 0) == 0, jnp.broadcast_to(value, (8, LANES)), 0.0)


def mixed_history(coeffs, history):
    left = left_half(1)
    c = [jnp.where(left_half(8), coeffs[i], coeffs[i + 4]) for i in range(4)]
    c24 = [jnp.concatenate([value] * 3, axis=0) for value in c]
    tiles = []
    for q in range(SIDE // 2):
        halves = []
        for m in (2 * q, 2 * q + 1):
            body = sum(history[pl.ds(PACKED * m + 24 * i, 24), :] * c24[i] for i in range(4))
            last = sum(history[pl.ds(PACKED * m + 96 + i, 1), :] * c[i][0:1] for i in range(4))
            halves.append((body + swap(body), last + swap(last)))
        body = jnp.where(left_half(24), halves[0][0], halves[1][0])
        last = jnp.where(left, halves[0][1], halves[1][1])
        tiles.append(jnp.concatenate([body, first_row(last)], axis=0))
    return tiles


def in_pairs(rows):
    left = left_half(1)
    return [jnp.where(left, swap(rows[2 * q]), rows[2 * q + 1]) for q in range(SIDE // 2)]


def known_slots(history):
    rows = [history[pl.ds(PACKED * m + NOTE, 1), :] for m in range(SIDE)]
    down = jnp.transpose(jnp.concatenate(rows, axis=0))[LANES - BATCHES :, :]
    return down, in_pairs(rows)


def to_targets(sums, out, rows):
    left = left_half(PIECE)
    for q in range(SIDE // 2):
        both = sums[:, q * LANES : (q + 1) * LANES]
        low, high = both[0:PIECE], both[PIECE : 2 * PIECE]
        out[pl.ds(2 * q * rows, PIECE), :] = jnp.where(left, low, swap(high))
        out[pl.ds((2 * q + 1) * rows, PIECE), :] = jnp.where(left, swap(low), high)


def first_route_kernel(history, rows, out, same, matrix_out, coeffs_out):
    note = history[NOTE : NOTE + 1, :]
    for m in range(1, SIDE):
        note = note + history[pl.ds(PACKED * m + NOTE, 1), :]
    matrix_out[...] = note
    coeffs = solve([[spread(note, HIST * i + j) for j in range(i + 1)] for i in range(HIST)])
    coeffs_out[...] = in_rows(coeffs)

    down, _ = known_slots(history)
    wanted = in_pairs([rows[m : m + 1, :] for m in range(SIDE)])
    for i in range(SIDE):
        mine = jnp.broadcast_to(down[:, i : i + 1], (BATCHES, LANES))
        for q in range(SIDE // 2):
            hit = jnp.where(mine == wanted[q], 1.0, 0.0)
            same[pl.ds(i * BATCHES, BATCHES), pl.ds(q * LANES, LANES)] = hit.astype(bf16)

    terms = split3(jnp.concatenate(mixed_history(coeffs, history), axis=1))
    to_targets(add_terms(jnp.dot(terms, same[...], preferred_element_type=f32)), out, PIECE)


def row_sum_kernel(pieces, out):
    row = pieces[PIECE - 1 : PIECE, :]
    for m in range(1, SIDE):
        row = row + pieces[pl.ds(PIECE * m + PIECE - 1, 1), :]
    out[...] = jnp.broadcast_to(row, (SIDE, LANES))


def last_route_kernel(
    where, place, rows, matrix_in, history, pieces, same, out, coeffs_out, low_hot
):
    slot, first = where[0], place[0]
    row = jnp.sum(rows[...], axis=0, keepdims=True)
    sub = iota((HIST, LANES), 0)
    old = matrix_in[...]
    new = [spread(row, BATCHES + i) for i in range(HIST)]
    coeffs = solve(
        [
            [
                jnp.where(slot == i, new[j], jnp.where(slot == j, new[i], spread(old, HIST * i + j)))
                for j in range(i + 1)
            ]
            for i in range(HIST)
        ]
    )
    coeffs_out[...] = in_rows(coeffs)
    fresh = jnp.where(slot == 0, coeffs[0], 0.0)
    for i in range(1, HIST):
        fresh = jnp.where(slot == i, coeffs[i], fresh)
    kept = [jnp.where(slot == i, 0.0, coeffs[i]) for i in range(HIST)]
    fresh = jnp.concatenate([fresh] * 4, axis=0)

    tiles = mixed_history(kept, history)
    left = left_half(PIECE)
    for q in range(SIDE // 2):
        a = pieces[pl.ds(PIECE * 2 * q, PIECE), :]
        b = pieces[pl.ds(PIECE * (2 * q + 1), PIECE), :]
        low = jnp.where(left, a, swap(b))
        high = jnp.where(left, swap(a), b)[: COMPS - PIECE]
        new = jnp.concatenate([low, high, jnp.zeros((32 - COMPS, LANES), f32)], axis=0)
        tiles[q] = tiles[q] + fresh * new
    terms = split3(jnp.concatenate(tiles, axis=1))
    to_targets(add_terms(jnp.dot(terms, same[...], preferred_element_type=f32)), out, FINAL)

    down, along = known_slots(history)
    low_bits = down.astype(jnp.int32) & 127
    for i in range(SIDE):
        mine = jnp.broadcast_to(low_bits[:, i : i + 1], (BATCHES, LANES))
        hit = jnp.where(mine == iota((BATCHES, LANES), 1), 1.0, 0.0)
        low_hot[pl.ds(i * BATCHES, BATCHES), :] = hit.astype(bf16)
    high_bits = jnp.concatenate(along, axis=1).astype(jnp.int32) >> 7
    masked = []
    for c in range(2):
        pick = jnp.where(high_bits == first + 4 * c, 1.0, 0.0)
        masked.append(terms * jnp.broadcast_to(pick, (96, KNOWN)).astype(bf16))
    product = jnp.dot(
        jnp.concatenate(masked, axis=0), low_hot[...], preferred_element_type=f32
    )
    for c in range(2):
        sums = add_terms(product[96 * c : 96 * c + 96])[0:COMPS]
        for z in range(SIDE // 2):
            out[pl.ds((2 * z + c) * FINAL + PIECE, COMPS), :] = sums


def at_batches(received, scales, rows):
    total = received[0:PIECE, :]
    for m in range(1, SIDE):
        total = total + received[pl.ds(rows * m, PIECE), :]
    high = swap(total)[: COMPS - PIECE]
    zero = jnp.zeros((32 - COMPS, LANES), f32)
    return jnp.concatenate([total, high, zero], axis=0) * scales


def damped(scale):
    k = iota((32, LANES), 0)
    value = jnp.full((32, LANES), float(damping_table[0]), f32)
    for degree in range(1, 5):
        value = jnp.where(k >= degree * degree, float(np.float32(1.0 / (1 + degree))), value)
    return jnp.where(k < COMPS, value * scale, 0.0)


def correction(at, b):
    return [
        jnp.broadcast_to(at[TOPS[t] : TOPS[t] + HEIGHTS[t], b : b + 1], (HEIGHTS[t], LANES))
        for t in range(4)
    ]


def correct_tile(wide, basis):
    terms = sum(wide[t] * basis[t] for t in range(3))
    return jnp.sum(terms, axis=0, keepdims=True) + wide[3] * basis[3]


def basis_tiles(basis, here):
    return [basis[pl.ds(TOPS[t], HEIGHTS[t]), here] for t in range(4)]


def update_kernel(
    scale, where, received, coeffs_in, basis, res, rho, weights, target, coupling,
    out, mixed_out, weighted,
):
    at = at_batches(received, damped(scale), PIECE)
    coeffs = coeffs_in[...]
    slot = where[0]
    sub = iota((HIST, LANES), 0)
    lane = iota((HIST, LANES), 1)
    overlap = jnp.zeros((HIST, LANES), f32)
    for b in range(BATCHES):
        wide = correction(at, b)
        for half in range(2):
            here = pl.ds(b * WIDTH + half * LANES, LANES)
            r = res[:, here]
            mixed = rho[:, here] + mixing_beta * r
            density = jnp.sum(coeffs * mixed, axis=0, keepdims=True)
            density = density - mixing_beta * correct_tile(wide, basis_tiles(basis, here))
            res_new = target[:, here] + coupling[:, here] * jnp.tanh(density) - density
            mixed_out[:, here] = jnp.where(sub == slot, density + mixing_beta * res_new, mixed)
            wr = weights[:, here] * res_new
            weighted[:, here] = wr
            overlap = overlap + jnp.where(sub == slot, res_new, r) * wr
    acc = [jnp.zeros((h, LANES), f32) for h in HEIGHTS]
    for b in range(BATCHES):
        total = [None] * 4
        for half in range(2):
            here = pl.ds(b * WIDTH + half * LANES, LANES)
            wr = weighted[:, here]
            y = basis_tiles(basis, here)
            for t in range(4):
                total[t] = y[t] * wr if half == 0 else total[t] + y[t] * wr
        for t in range(4):
            sums = jnp.sum(total[t], axis=1, keepdims=True)
            acc[t] = jnp.where(lane[: HEIGHTS[t]] == b, sums, acc[t])
    sums = jnp.sum(overlap, axis=1, keepdims=True)
    row = jnp.sum(jnp.where(lane == sub, sums, 0.0), axis=0, keepdims=True)
    full = jnp.concatenate([acc[0], acc[1], acc[2], acc[3], row], axis=0)
    packed = full[0:PIECE] + swap(full[PIECE : 2 * PIECE])
    for peer in range(SIDE):
        out[pl.ds(PIECE * peer, PIECE), :] = packed


def quarter_kernel(scale, received, out):
    total = received[PIECE:FINAL, :]
    for m in range(1, SIDE):
        total = total + received[pl.ds(FINAL * m + PIECE, COMPS), :]
    out[0:COMPS, :] = total * scale
    out[COMPS:32, :] = jnp.zeros((32 - COMPS, LANES), f32)


def density_kernel(scale, received, coeffs_in, basis, mixed, density_out):
    at = at_batches(received, damped(scale), FINAL)
    coeffs = coeffs_in[...]
    for b in range(BATCHES):
        wide = correction(at, b)
        for half in range(2):
            here = pl.ds(b * WIDTH + half * LANES, LANES)
            density = jnp.sum(coeffs * mixed[:, here], axis=0, keepdims=True)
            correct = correct_tile(wide, basis_tiles(basis, here))
            density_out[:, here] = density - mixing_beta * correct


def owned_kernel(place, mine, one, two, three, moments_out):
    y = place[1]
    for step, quarter in enumerate((mine, one, two, three)):
        at = pl.multiple_of(((y + 4 - step) & 3) * QUARTER, QUARTER)
        moments_out[:, pl.ds(at, QUARTER)] = quarter[0:COMPS, :]


def exchange(pieces, axes):
    rows = pieces.reshape(-1, 1, LANES)
    return lax.all_to_all(rows, axes, 0, 0, tiled=True).reshape(-1, LANES)


def local(
    weights,
    target,
    coupling,
    multipole_basis,
    rho_hist,
    res_hist,
    batch_atom,
    owner_slot,
    slot_index,
):
    points = weights.shape[0]
    owned_count = owner_slot.shape[0] // lax.axis_size(ATOM)
    atom_points = points * lax.axis_size(GRID) // owned_count
    scale = 1.0 / math.sqrt(atom_points)
    assert points == POINTS and owned_count == OWNED and multipole_basis.shape[0] == COMPS

    weights, target, coupling = (v.reshape(1, points) for v in (weights, target, coupling))
    atoms = batch_atom.reshape(1, BATCHES)
    table = owner_slot.reshape(-1, LANES)
    y = lax.axis_index("y").astype(jnp.int32)
    place = jnp.stack([lax.axis_index("x").astype(jnp.int32) * 8 + y, y])
    atoms, place, where = lax.optimization_barrier((atoms, place, slot_index[0:1]))

    sent, res_hist, weights = call(
        gram_kernel,
        (shape(1, LANES), shape(HIST, POINTS), shape(1, POINTS)),
        [pltpu.HBM] * 4,
        scratch=[
            pltpu.VMEM((1, BATCHES), jnp.int32),
            pltpu.VMEM((32, LANES), jnp.int32),
            pltpu.SemaphoreType.DMA((4 + PARTS,)),
        ],
    )(*(
        pltpu.with_memory_space_constraint(v, pltpu.HBM)
        for v in (res_hist, weights, atoms, table)
    ))
    rows = call(repeat_kernel, shape(SIDE, LANES), [V], cost=6000000)(sent)
    rows = exchange(rows, COL)
    history = call(
        history_moments_kernel,
        shape(SIDE * PACKED, LANES),
        [V] * 5,
        scratch=[pltpu.VMEM((104, LANES), f32)],
    )(res_hist, weights, multipole_basis, sent, rows)
    history = exchange(history, ROW)
    pieces, same, matrix, coeffs = call(
        first_route_kernel,
        (
            shape(SIDE * PIECE, LANES),
            shape(KNOWN, KNOWN, dtype=bf16),
            shape(1, LANES),
            shape(HIST, LANES),
        ),
        [V] * 2,
    )(history, rows)
    received = exchange(pieces, COL)

    pieces, mixed = call(
        functools.partial(update_kernel, scale),
        (shape(SIDE * PIECE, LANES), shape(HIST, POINTS)),
        [S] + [V] * 8,
        scratch=[pltpu.VMEM((1, POINTS), f32)],
    )(where, received, coeffs, multipole_basis, res_hist, rho_hist, weights, target, coupling)
    pieces = exchange(pieces, ROW)
    rows = call(row_sum_kernel, shape(SIDE, LANES), [V])(pieces)
    rows = exchange(rows, COL)
    routed, coeffs = call(
        last_route_kernel,
        (shape(SIDE * FINAL, LANES), shape(HIST, LANES)),
        [S, S] + [V] * 5,
        scratch=[pltpu.VMEM((KNOWN, LANES), bf16)],
    )(where, place, rows, matrix, history, pieces, same)
    received = exchange(routed, COL)
    mine = call(functools.partial(quarter_kernel, scale), shape(32, LANES), [V])(received)
    others = [
        lax.ppermute(mine, "y", [(i, (i + step) % 4) for i in range(4)]) for step in (1, 2, 3)
    ]
    density = call(functools.partial(density_kernel, scale), shape(1, POINTS), [V] * 4)(
        received, coeffs, multipole_basis, mixed
    )
    moments = call(owned_kernel, shape(COMPS, OWNED), [S] + [V] * 4)(place, mine, *others)
    return density.reshape(points), moments


def solution(mesh):
    torus = Mesh(mesh.devices.reshape(8, 4, 4, 2), AXES)
    placed = (
        P(AXES),
        P(AXES),
        P(AXES),
        P(None, AXES),
        P(None, AXES),
        P(None, AXES),
        P(AXES),
        P(),
        P(),
    )
    return jax.shard_map(
        local, mesh=torus, in_specs=placed, out_specs=(P(AXES), P(None, ATOM)), check_vma=False
    )
```

```python
import functools
import math

import jax
import jax.numpy as jnp
import numpy as np
from jax import lax
from jax.experimental import pallas as pl
from jax.experimental.pallas import tpu as pltpu
from jax.sharding import Mesh
from jax.sharding import PartitionSpec as P

ITERS = 2
AXES = ("z", "y", "x", "c")
GRID = ("z", "y")
ATOM = ("x", "c")
COL = ("z", "c")
ROW = ("y", "x")

damping_table = np.array(
    [1.0 / (1 + degree) for degree in range(5) for order in range(2 * degree + 1)], dtype=np.float32
)
mixing_beta = 0.5
ridge_share = 0.1

LANES = 128
HIST = 8
COMPS = 25
BATCHES = 64
WIDTH = 256
POINTS = BATCHES * WIDTH
SIDE = 16
KNOWN = SIDE * BATCHES
OWNED = 512
PIECE = 13
NOTE = 100
PACKED = 101
FINAL = 38
QUARTER = OWNED // 4
PARTS = 4

f32 = jnp.float32
bf16 = jnp.bfloat16


def iota(shape, dim):
    return lax.broadcasted_iota(jnp.int32, shape, dim)


def call(kernel, out_shape, in_specs, *, scratch=(), vmem=12 << 20, cost=20000):
    return pl.pallas_call(
        kernel,
        out_shape=out_shape,
        in_specs=[pl.BlockSpec(memory_space=s) for s in in_specs],
        out_specs=jax.tree.map(lambda _: pl.BlockSpec(memory_space=pltpu.VMEM), out_shape),
        scratch_shapes=list(scratch),
        compiler_params=pltpu.CompilerParams(vmem_limit_bytes=vmem),
        cost_estimate=pl.CostEstimate(flops=cost * 1000, bytes_accessed=1 << 20, transcendentals=0),
    )


V = pltpu.VMEM
S = pltpu.SMEM


def shape(*dims, dtype=f32):
    return jax.ShapeDtypeStruct(dims, dtype)


TOPS = (0, 8, 16, 24)
HEIGHTS = (8, 8, 8, 1)


def left_half(rows):
    return iota((rows, LANES), 1) < BATCHES


def swap(value):
    return pltpu.roll(value, BATCHES, 1)


def slots_of(atoms, table):
    hits = jnp.where(iota((32, BATCHES), 0) == (atoms >> 7), 1.0, 0.0).astype(bf16)
    halves = []
    for half in (table >> 6, table & 63):
        rows = lax.dot_general(
            half.astype(f32).astype(bf16), hits, (((0,), (0,)), ((), ())),
            preferred_element_type=f32,
        )
        mine = iota((LANES, BATCHES), 0) == (atoms & 127)
        halves.append(jnp.sum(jnp.where(mine, rows, 0.0), axis=0, keepdims=True))
    return halves[0] * 64.0 + halves[1]


def gram_kernel(
    res_in, weights_in, atoms_in, table_in,
    out, res, weights,
    atoms, table, sems,
):
    def fetch(source, target, sem):
        copy = pltpu.make_async_copy(source, target, sems.at[sem])
        copy.start()
        return copy

    step = POINTS // PARTS
    fetches = [fetch(weights_in, weights, 0)]
    for part in range(PARTS):
        at = (slice(None), pl.ds(part * step, step))
        fetches.append(fetch(res_in.at[at], res.at[at], 1 + part))
    small = [fetch(atoms_in, atoms, 1 + PARTS), fetch(table_in, table, 2 + PARTS)]

    acc = [jnp.zeros((HIST, LANES), f32) for _ in range(5)]
    fetches[0].wait()
    for part in range(PARTS):
        fetches[1 + part].wait()
        for tile in range(step // LANES):
            at = pl.ds(part * step + tile * LANES, LANES)
            r = res[:, at]
            rw = r * weights[:, at]
            acc[0] += rw * r
            for d in range(1, 5):
                acc[d] += rw * pltpu.roll(r, HIST - d, 0)
    for copy in small:
        copy.wait()
    lane = iota((HIST, LANES), 1)
    sub = iota((HIST, LANES), 0)
    placed = jnp.zeros((HIST, LANES), f32)
    for d in range(HIST):
        if d < 5:
            sums = jnp.broadcast_to(jnp.sum(acc[d], axis=1, keepdims=True), (HIST, LANES))
        else:
            sums = jnp.broadcast_to(jnp.sum(acc[HIST - d], axis=1, keepdims=True), (HIST, LANES))
            sums = pltpu.roll(sums, HIST - d, 0)
        here = ((lane >> 3) == sub) & ((lane & 7) == ((sub + d) & 7))
        placed = jnp.where(here, sums, placed)
    slots = slots_of(atoms[...], table[...])
    slots = jnp.concatenate([jnp.zeros((1, BATCHES), f32), slots], axis=1)
    out[...] = jnp.sum(placed, axis=0, keepdims=True) + slots


def repeat_kernel(row, out):
    out[...] = jnp.broadcast_to(row[...], (SIDE, LANES))


def history_moments_kernel(res, weights, basis, sent, rows, out, whole):
    lane = iota((HIST, LANES), 1)
    ends = jnp.zeros((HIST, LANES), f32)
    for i4 in range(4):
        acc = [jnp.zeros((HIST, LANES), f32) for _ in range(3)]
        for b in range(BATCHES):
            at = [pl.ds(b * WIDTH + half * LANES, LANES) for half in range(2)]
            for i in (i4, i4 + 4):
                wr = [res[i : i + 1, h] * weights[:, h] for h in at]
                place = b if i < 4 else b + BATCHES
                for t in range(3):
                    rows_t = pl.ds(TOPS[t], 8)
                    total = basis[rows_t, at[0]] * wr[0] + basis[rows_t, at[1]] * wr[1]
                    sums = jnp.sum(total, axis=1, keepdims=True)
                    acc[t] = jnp.where(lane == place, sums, acc[t])
            if i4 == 0:
                total = sum(res[:, h] * (weights[:, h] * basis[24:25, h]) for h in at)
                sums = jnp.sum(total, axis=1, keepdims=True)
                ends = jnp.where(lane == b, sums, ends)
        for t in range(3):
            whole[pl.ds(24 * i4 + 8 * t, 8), :] = acc[t]
    whole[pl.ds(96, 8), :] = jnp.where(
        iota((8, LANES), 0) < 4, ends + pltpu.roll(swap(ends), 4, 0), 0.0
    )
    note = jnp.sum(rows[...], axis=0, keepdims=True)
    whole[NOTE : NOTE + 1, :] = jnp.where(left_half(1), note, sent[...])
    for peer in range(SIDE):
        out[PACKED * peer : PACKED * (peer + 1), :] = whole[0:PACKED, :]


def spread(row, lane):
    return jnp.broadcast_to(row[:, lane : lane + 1], (HIST, LANES))


def solve(matrix):
    trace = matrix[0][0]
    for i in range(1, HIST):
        trace = trace + matrix[i][i]
    ridge = ridge_share * trace / HIST
    m = [[matrix[i][j] + ridge if i == j else matrix[i][j] for j in range(i + 1)] for i in range(HIST)]
    right = [jnp.ones((HIST, LANES), f32)] * HIST
    inverse = []
    for j in range(HIST):
        inverse.append(1.0 / m[j][j])
        for i in range(j + 1, HIST):
            factor = m[i][j] * inverse[j]
            right[i] = right[i] - factor * right[j]
            for k in range(j + 1, i + 1):
                m[i][k] = m[i][k] - factor * m[k][j]
    z = [None] * HIST
    for j in reversed(range(HIST)):
        value = right[j]
        for i in range(j + 1, HIST):
            value = value - m[i][j] * z[i]
        z[j] = value * inverse[j]
    total = z[0]
    for j in range(1, HIST):
        total = total + z[j]
    return [value / total for value in z]


def in_rows(coeffs):
    sub = iota((HIST, LANES), 0)
    rows = coeffs[0]
    for i in range(1, HIST):
        rows = jnp.where(sub == i, coeffs[i], rows)
    return rows


def split3(value):
    hi = value.astype(bf16)
    rest = value - hi.astype(f32)
    mid = rest.astype(bf16)
    lo = (rest - mid.astype(f32)).astype(bf16)
    return jnp.concatenate([hi, mid, lo], axis=0)


def add_terms(product):
    return product[0:32] + product[32:64] + product[64:96]


def first_row(value):
    return jnp.where(iota((8, LANES), 0) == 0, jnp.broadcast_to(value, (8, LANES)), 0.0)


def mixed_history(coeffs, history):
    left = left_half(1)
    c = [jnp.where(left_half(8), coeffs[i], coeffs[i + 4]) for i in range(4)]
    c24 = [jnp.concatenate([value] * 3, axis=0) for value in c]
    tiles = []
    for q in range(SIDE // 2):
        halves = []
        for m in (2 * q, 2 * q + 1):
            body = sum(history[pl.ds(PACKED * m + 24 * i, 24), :] * c24[i] for i in range(4))
            last = sum(history[pl.ds(PACKED * m + 96 + i, 1), :] * c[i][0:1] for i in range(4))
            halves.append((body + swap(body), last + swap(last)))
        body = jnp.where(left_half(24), halves[0][0], halves[1][0])
        last = jnp.where(left, halves[0][1], halves[1][1])
        tiles.append(jnp.concatenate([body, first_row(last)], axis=0))
    return tiles


def in_pairs(rows):
    left = left_half(1)
    return [jnp.where(left, swap(rows[2 * q]), rows[2 * q + 1]) for q in range(SIDE // 2)]


def known_slots(history):
    rows = [history[pl.ds(PACKED * m + NOTE, 1), :] for m in range(SIDE)]
    down = jnp.transpose(jnp.concatenate(rows, axis=0))[LANES - BATCHES :, :]
    return down, in_pairs(rows)


def to_targets(sums, out, rows):
    left = left_half(PIECE)
    for q in range(SIDE // 2):
        both = sums[:, q * LANES : (q + 1) * LANES]
        low, high = both[0:PIECE], both[PIECE : 2 * PIECE]
        out[pl.ds(2 * q * rows, PIECE), :] = jnp.where(left, low, swap(high))
        out[pl.ds((2 * q + 1) * rows, PIECE), :] = jnp.where(left, swap(low), high)


def first_route_kernel(history, rows, out, same, matrix_out, coeffs_out):
    note = history[NOTE : NOTE + 1, :]
    for m in range(1, SIDE):
        note = note + history[pl.ds(PACKED * m + NOTE, 1), :]
    matrix_out[...] = note
    coeffs = solve([[spread(note, HIST * i + j) for j in range(i + 1)] for i in range(HIST)])
    coeffs_out[...] = in_rows(coeffs)

    down, _ = known_slots(history)
    wanted = in_pairs([rows[m : m + 1, :] for m in range(SIDE)])
    for i in range(SIDE):
        mine = jnp.broadcast_to(down[:, i : i + 1], (BATCHES, LANES))
        for q in range(SIDE // 2):
            hit = jnp.where(mine == wanted[q], 1.0, 0.0)
            same[pl.ds(i * BATCHES, BATCHES), pl.ds(q * LANES, LANES)] = hit.astype(bf16)

    terms = split3(jnp.concatenate(mixed_history(coeffs, history), axis=1))
    to_targets(add_terms(jnp.dot(terms, same[...], preferred_element_type=f32)), out, PIECE)


def row_sum_kernel(pieces, out):
    row = pieces[PIECE - 1 : PIECE, :]
    for m in range(1, SIDE):
        row = row + pieces[pl.ds(PIECE * m + PIECE - 1, 1), :]
    out[...] = jnp.broadcast_to(row, (SIDE, LANES))


def last_route_kernel(
    where, place, rows, matrix_in, history, pieces, same, out, coeffs_out, low_hot
):
    slot, first = where[0], place[0]
    row = jnp.sum(rows[...], axis=0, keepdims=True)
    sub = iota((HIST, LANES), 0)
    old = matrix_in[...]
    new = [spread(row, BATCHES + i) for i in range(HIST)]
    coeffs = solve(
        [
            [
                jnp.where(slot == i, new[j], jnp.where(slot == j, new[i], spread(old, HIST * i + j)))
                for j in range(i + 1)
            ]
            for i in range(HIST)
        ]
    )
    coeffs_out[...] = in_rows(coeffs)
    fresh = jnp.where(slot == 0, coeffs[0], 0.0)
    for i in range(1, HIST):
        fresh = jnp.where(slot == i, coeffs[i], fresh)
    kept = [jnp.where(slot == i, 0.0, coeffs[i]) for i in range(HIST)]
    fresh = jnp.concatenate([fresh] * 4, axis=0)

    tiles = mixed_history(kept, history)
    left = left_half(PIECE)
    for q in range(SIDE // 2):
        a = pieces[pl.ds(PIECE * 2 * q, PIECE), :]
        b = pieces[pl.ds(PIECE * (2 * q + 1), PIECE), :]
        low = jnp.where(left, a, swap(b))
        high = jnp.where(left, swap(a), b)[: COMPS - PIECE]
        new = jnp.concatenate([low, high, jnp.zeros((32 - COMPS, LANES), f32)], axis=0)
        tiles[q] = tiles[q] + fresh * new
    terms = split3(jnp.concatenate(tiles, axis=1))
    to_targets(add_terms(jnp.dot(terms, same[...], preferred_element_type=f32)), out, FINAL)

    down, along = known_slots(history)
    low_bits = down.astype(jnp.int32) & 127
    for i in range(SIDE):
        mine = jnp.broadcast_to(low_bits[:, i : i + 1], (BATCHES, LANES))
        hit = jnp.where(mine == iota((BATCHES, LANES), 1), 1.0, 0.0)
        low_hot[pl.ds(i * BATCHES, BATCHES), :] = hit.astype(bf16)
    high_bits = jnp.concatenate(along, axis=1).astype(jnp.int32) >> 7
    masked = []
    for c in range(2):
        pick = jnp.where(high_bits == first + 4 * c, 1.0, 0.0)
        masked.append(terms * jnp.broadcast_to(pick, (96, KNOWN)).astype(bf16))
    product = jnp.dot(
        jnp.concatenate(masked, axis=0), low_hot[...], preferred_element_type=f32
    )
    for c in range(2):
        sums = add_terms(product[96 * c : 96 * c + 96])[0:COMPS]
        for z in range(SIDE // 2):
            out[pl.ds((2 * z + c) * FINAL + PIECE, COMPS), :] = sums


def at_batches(received, scales, rows):
    total = received[0:PIECE, :]
    for m in range(1, SIDE):
        total = total + received[pl.ds(rows * m, PIECE), :]
    high = swap(total)[: COMPS - PIECE]
    zero = jnp.zeros((32 - COMPS, LANES), f32)
    return jnp.concatenate([total, high, zero], axis=0) * scales


def damped(scale):
    k = iota((32, LANES), 0)
    value = jnp.full((32, LANES), float(damping_table[0]), f32)
    for degree in range(1, 5):
        value = jnp.where(k >= degree * degree, float(np.float32(1.0 / (1 + degree))), value)
    return jnp.where(k < COMPS, value * scale, 0.0)


def correction(at, b):
    return [
        jnp.broadcast_to(at[TOPS[t] : TOPS[t] + HEIGHTS[t], b : b + 1], (HEIGHTS[t], LANES))
        for t in range(4)
    ]


def correct_tile(wide, basis):
    terms = sum(wide[t] * basis[t] for t in range(3))
    return jnp.sum(terms, axis=0, keepdims=True) + wide[3] * basis[3]


def basis_tiles(basis, here):
    return [basis[pl.ds(TOPS[t], HEIGHTS[t]), here] for t in range(4)]


def update_kernel(
    scale, where, received, coeffs_in, basis, res, rho, weights, target, coupling,
    out, mixed_out, weighted,
):
    at = at_batches(received, damped(scale), PIECE)
    coeffs = coeffs_in[...]
    slot = where[0]
    sub = iota((HIST, LANES), 0)
    lane = iota((HIST, LANES), 1)
    overlap = jnp.zeros((HIST, LANES), f32)
    for b in range(BATCHES):
        wide = correction(at, b)
        for half in range(2):
            here = pl.ds(b * WIDTH + half * LANES, LANES)
            r = res[:, here]
            mixed = rho[:, here] + mixing_beta * r
            density = jnp.sum(coeffs * mixed, axis=0, keepdims=True)
            density = density - mixing_beta * correct_tile(wide, basis_tiles(basis, here))
            res_new = target[:, here] + coupling[:, here] * jnp.tanh(density) - density
            mixed_out[:, here] = jnp.where(sub == slot, density + mixing_beta * res_new, mixed)
            wr = weights[:, here] * res_new
            weighted[:, here] = wr
            overlap = overlap + jnp.where(sub == slot, res_new, r) * wr
    acc = [jnp.zeros((h, LANES), f32) for h in HEIGHTS]
    for b in range(BATCHES):
        total = [None] * 4
        for half in range(2):
            here = pl.ds(b * WIDTH + half * LANES, LANES)
            wr = weighted[:, here]
            y = basis_tiles(basis, here)
            for t in range(4):
                total[t] = y[t] * wr if half == 0 else total[t] + y[t] * wr
        for t in range(4):
            sums = jnp.sum(total[t], axis=1, keepdims=True)
            acc[t] = jnp.where(lane[: HEIGHTS[t]] == b, sums, acc[t])
    sums = jnp.sum(overlap, axis=1, keepdims=True)
    row = jnp.sum(jnp.where(lane == sub, sums, 0.0), axis=0, keepdims=True)
    full = jnp.concatenate([acc[0], acc[1], acc[2], acc[3], row], axis=0)
    packed = full[0:PIECE] + swap(full[PIECE : 2 * PIECE])
    for peer in range(SIDE):
        out[pl.ds(PIECE * peer, PIECE), :] = packed


def quarter_kernel(scale, received, out):
    total = received[PIECE:FINAL, :]
    for m in range(1, SIDE):
        total = total + received[pl.ds(FINAL * m + PIECE, COMPS), :]
    out[0:COMPS, :] = total * scale
    out[COMPS:32, :] = jnp.zeros((32 - COMPS, LANES), f32)


def density_kernel(scale, received, coeffs_in, basis, mixed, density_out):
    at = at_batches(received, damped(scale), FINAL)
    coeffs = coeffs_in[...]
    for b in range(BATCHES):
        wide = correction(at, b)
        for half in range(2):
            here = pl.ds(b * WIDTH + half * LANES, LANES)
            density = jnp.sum(coeffs * mixed[:, here], axis=0, keepdims=True)
            correct = correct_tile(wide, basis_tiles(basis, here))
            density_out[:, here] = density - mixing_beta * correct


def owned_kernel(place, mine, one, two, three, moments_out):
    y = place[1]
    for step, quarter in enumerate((mine, one, two, three)):
        at = pl.multiple_of(((y + 4 - step) & 3) * QUARTER, QUARTER)
        moments_out[:, pl.ds(at, QUARTER)] = quarter[0:COMPS, :]


def exchange(pieces, axes):
    rows = pieces.reshape(-1, 1, LANES)
    return lax.all_to_all(rows, axes, 0, 0, tiled=True).reshape(-1, LANES)


def local(
    weights,
    target,
    coupling,
    multipole_basis,
    rho_hist,
    res_hist,
    batch_atom,
    owner_slot,
    slot_index,
):
    points = weights.shape[0]
    owned_count = owner_slot.shape[0] // lax.axis_size(ATOM)
    atom_points = points * lax.axis_size(GRID) // owned_count
    scale = 1.0 / math.sqrt(atom_points)
    assert points == POINTS and owned_count == OWNED and multipole_basis.shape[0] == COMPS

    weights, target, coupling = (v.reshape(1, points) for v in (weights, target, coupling))
    atoms = batch_atom.reshape(1, BATCHES)
    table = owner_slot.reshape(-1, LANES)
    y = lax.axis_index("y").astype(jnp.int32)
    place = jnp.stack([lax.axis_index("x").astype(jnp.int32) * 8 + y, y])
    atoms, place, where = lax.optimization_barrier((atoms, place, slot_index[0:1]))

    sent, res_hist, weights = call(
        gram_kernel,
        (shape(1, LANES), shape(HIST, POINTS), shape(1, POINTS)),
        [pltpu.HBM] * 4,
        scratch=[
            pltpu.VMEM((1, BATCHES), jnp.int32),
            pltpu.VMEM((32, LANES), jnp.int32),
            pltpu.SemaphoreType.DMA((4 + PARTS,)),
        ],
    )(*(
        pltpu.with_memory_space_constraint(v, pltpu.HBM)
        for v in (res_hist, weights, atoms, table)
    ))
    rows = call(repeat_kernel, shape(SIDE, LANES), [V], cost=6000000)(sent)
    rows = exchange(rows, COL)
    history = call(
        history_moments_kernel,
        shape(SIDE * PACKED, LANES),
        [V] * 5,
        scratch=[pltpu.VMEM((104, LANES), f32)],
    )(res_hist, weights, multipole_basis, sent, rows)
    history = exchange(history, ROW)
    pieces, same, matrix, coeffs = call(
        first_route_kernel,
        (
            shape(SIDE * PIECE, LANES),
            shape(KNOWN, KNOWN, dtype=bf16),
            shape(1, LANES),
            shape(HIST, LANES),
        ),
        [V] * 2,
    )(history, rows)
    received = exchange(pieces, COL)

    pieces, mixed = call(
        functools.partial(update_kernel, scale),
        (shape(SIDE * PIECE, LANES), shape(HIST, POINTS)),
        [S] + [V] * 8,
        scratch=[pltpu.VMEM((1, POINTS), f32)],
    )(where, received, coeffs, multipole_basis, res_hist, rho_hist, weights, target, coupling)
    pieces = exchange(pieces, ROW)
    rows = call(row_sum_kernel, shape(SIDE, LANES), [V])(pieces)
    rows = exchange(rows, COL)
    routed, coeffs = call(
        last_route_kernel,
        (shape(SIDE * FINAL, LANES), shape(HIST, LANES)),
        [S, S] + [V] * 5,
        scratch=[pltpu.VMEM((KNOWN, LANES), bf16)],
    )(where, place, rows, matrix, history, pieces, same)
    received = exchange(routed, COL)
    mine = call(functools.partial(quarter_kernel, scale), shape(32, LANES), [V])(received)
    others = [
        lax.ppermute(mine, "y", [(i, (i + step) % 4) for i in range(4)]) for step in (1, 2, 3)
    ]
    density = call(functools.partial(density_kernel, scale), shape(1, POINTS), [V] * 4)(
        received, coeffs, multipole_basis, mixed
    )
    moments = call(owned_kernel, pltpu.VMEM((COMPS, OWNED), f32), [S] + [V] * 4)(place, mine, *others)
    return density.reshape(points), moments


def solution(mesh):
    torus = Mesh(mesh.devices.reshape(8, 4, 4, 2), AXES)
    placed = (
        P(AXES),
        P(AXES),
        P(AXES),
        P(None, AXES),
        P(None, AXES),
        P(None, AXES),
        P(AXES),
        P(),
        P(),
    )
    return jax.shard_map(
        local, mesh=torus, in_specs=placed, out_specs=(P(AXES), P(None, ATOM)), check_vma=False
    )
```
